32 devices in a mesh: row: 8 (over y, x, core), col: 4 (over z).
Axes of the slice: x: 2, y: 2, z: 4, core: 2. Of those that a mesh axis runs over, the one named last changes fastest.
Arguments:
- tokens: bfloat16 [4096, 2048], P(('row', 'col')), may hold values from -30 to 30
- ln1_gain: float32 [2048], replicated, may hold values from 0.25 to 1.75
- qkv_weight: bfloat16 [2048, 16, 3, 128], P('row', 'col'), may hold values from -4 to 4
- out_weight: bfloat16 [2048, 2048], P('col', 'row'), may hold values from -0.125 to 0.125
- ln2_gain: float32 [2048], replicated, may hold values from 0.25 to 1.75
- ffn_in: bfloat16 [2048, 8192], P('row', 'col'), may hold values from -0.125 to 0.125
- ffn_out: bfloat16 [8192, 2048], P('col', 'row'), may hold values from -0.0625 to 0.0625
- expert_ids: int32 [4096, 1], P(('row', 'col')), may hold values from 0 to 15; in each aligned block of 128 rows (0 to 127, 128 to 255, ...) at most 16 rows name the same one
- expert_in: bfloat16 [32, 2048, 2048], P(('row', 'col')), may hold values from -0.125 to 0.125
- expert_out: bfloat16 [32, 2048, 2048], P(('row', 'col')), may hold values from -0.09375 to 0.09375
Outputs:
- block_out: bfloat16 [4096, 2048], P(('row', 'col'))
The draws below stay inside these ranges and needn't reach their ends.
Inputs may be any that keep to these rules, and one draw needn't show every extreme that they name: `expert_ids`: among the tokens of one device no expert is named more than 16 times, and in every draw some expert is named exactly 16 times by the tokens of some device.
All inputs are finite; a program needn't handle non-finite values.
Results may differ from the reference program's by a relative error of at most 0.013.
Values may be sent and summed in bfloat16 or wider, within the bound.
A program may use at most 128 MiB of HBM per device.

```python
import math
import jax
import jax.numpy as jnp
import numpy as np
from jax import lax

D = 2048
HEADS = 16
DH = 128
FF = 8192
FFE = 4096
TOK_DEV = 128
SEQ = 512
TOKENS = 4096
EXPERTS = 16
CAP = 16
FF_BLOCK = 2048
HALF = 2048
N_ROW = 8
N_COL = 4


def draw_tokens(key, part):
    first_key = jax.random.fold_in(jax.random.fold_in(key, 11), 0)
    base_values = jax.random.normal(first_key, (TOKENS, D), jnp.float32)
    return jnp.clip(base_values, -30.0, 30.0).astype(jnp.bfloat16)


def draw_qkv_weight(key, part):
    first_key = jax.random.fold_in(jax.random.fold_in(key, 23), 0)
    base_values = jax.random.normal(first_key, (D, HEADS, 3, DH), jnp.float32) * D ** (-0.5)
    factors = jnp.array([2.0, 1.0, 1.0], jnp.float32)[None, None, :, None]
    base_values = base_values * factors
    return jnp.clip(base_values, -4.0, 4.0).astype(jnp.bfloat16)


def block_scale(key, dims, shards, low, high):
    gain, own = 1.0, jax.random.fold_in(key, 6)
    for dim, blocks in shards:
        draws = jnp.exp(jax.random.uniform(jax.random.fold_in(own, dim), (blocks,), jnp.float32, low / len(shards), high / len(shards)))
        gain = gain * jnp.repeat(draws, dims[dim] // blocks).reshape([-1 if axis == dim else 1 for axis in range(len(dims))])
    return gain


def assign_block(key, own, number, rows, count, top, reach, slope):
    ranking = jax.random.permutation(key, count)
    crowded, common = portions_of(count, rows * top, reach, slope, True), portions_of(count, rows * top, reach, slope, False)
    places = jnp.arange(count)

    def named(lengths, offset_by):
        used = int((lengths > 0).sum())
        fixed = max(1, used // 4)
        passed = fixed + (places - fixed + offset_by * (used - fixed)) % max(1, count - fixed)
        return jnp.zeros((count,), jnp.int32).at[ranking[jnp.where(places < fixed, places, passed)]].set(jnp.asarray(lengths, jnp.int32))

    lengths = jnp.where(number % 4 == 0, named(crowded, number // 4), named(common, number - number // 4 - 1))
    mixed = jax.random.permutation(jax.random.fold_in(own, 3), count)
    giver, receiver = mixed[0:count // 2 * 2:2], mixed[1:count // 2 * 2:2]
    margin = jnp.minimum(lengths[giver] - 1, reach - lengths[receiver]) // 2
    margin = jnp.where((giver == ranking[0]) | (receiver == ranking[0]) | (lengths[receiver] == 0), 0, jnp.maximum(margin, 0))
    passed = jax.random.randint(jax.random.fold_in(own, 4), (count // 2,), 0, 1 << 20) % (margin + 1)
    lengths = lengths.at[giver].add(-passed).at[receiver].add(passed)
    members = jnp.searchsorted(jnp.cumsum(lengths), jnp.arange(rows * top), side="right").astype(jnp.int32)
    grid = members.reshape(top, rows).T
    grid = grid[jax.random.permutation(jax.random.fold_in(own, 1), rows)]
    offset_by = jax.random.randint(jax.random.fold_in(own, 2), (rows, 1), 0, top)
    return jnp.take_along_axis(grid, (jnp.arange(top)[None, :] + offset_by) % top, axis=1)


def portions_of(count, total, limit, skew, full):
    weights = [(1 << 20) // math.isqrt(rank ** skew) + 1 for rank in range(1, count + 1)]
    largest = limit if full else min(limit, max(-(-total // count), total * weights[0] // sum(weights)))
    least = 1 if total - largest >= count - 1 else 0
    holding, rest = [largest] + [least] * (count - 1), total - largest - least * (count - 1)
    while rest > 0:
        candidates = [i for i in range(1, count) if holding[i] < largest] or [i for i in range(1, count) if holding[i] < limit]
        whole, remaining = sum([weights[i] for i in candidates]), rest
        for i in candidates:
            extra = min(limit - holding[i], max(1, remaining * weights[i] // whole), rest)
            holding[i] = holding[i] + extra
            rest = rest - extra
    return np.array(holding)


def normal_values(own_key, dims, width, bound, pieces=(), held_as=jnp.bfloat16):
    factor_of = block_scale(own_key, dims, pieces, -0.22, 0.18) if pieces else 1.0
    values = jax.random.normal(own_key, dims, jnp.float32) * width * factor_of
    return jnp.minimum(jnp.maximum(values, -bound), bound).astype(held_as)


def setup_inputs(seed: int = 0) -> dict:
    key_list = jax.random.split(jax.random.key(seed), 11)
    tokens = draw_tokens(jax.random.fold_in(key_list[10], 71), 0)
    ln1_gain = jnp.clip(1.0 + 0.15 * jax.random.normal(key_list[1], (D,), jnp.float32), 0.25, 1.75)
    qkv_weight = draw_qkv_weight(jax.random.fold_in(key_list[10], 71), 0)
    out_weight = normal_values(key_list[3], (HEADS * DH, D), (HEADS * DH) ** -0.5, 0.125, ((0, 4), (1, 8)))
    ln2_gain = jnp.clip(1.0 + 0.15 * jax.random.normal(key_list[4], (D,), jnp.float32), 0.25, 1.75)
    ffn_in = normal_values(key_list[5], (D, FF), D ** -0.5, 0.125, ((0, 8), (1, 4)))
    ffn_out = normal_values(key_list[6], (FF, D), FF ** -0.5, 0.0625, ((0, 4), (1, 8)))
    expert_ids_keys = jax.random.split(jax.random.fold_in(key_list[7], 1), TOKENS // TOK_DEV)
    expert_ids_turns = jax.random.permutation(jax.random.fold_in(key_list[7], 3), TOKENS // TOK_DEV)
    expert_ids = jax.vmap(lambda own, number: assign_block(jax.random.fold_in(key_list[7], 2), own, number, TOK_DEV, EXPERTS, 1, CAP, 2))(expert_ids_keys, expert_ids_turns).reshape((TOKENS, 1))
    expert_in = normal_values(key_list[8], (EXPERTS * 2, D, HALF), D ** -0.5, 0.125, ((0, 32),))
    expert_out = normal_values(key_list[9], (EXPERTS * 2, HALF, D), FFE ** -0.5, 0.09375, ((0, 32),))
    return {"tokens": tokens, "ln1_gain": ln1_gain, "qkv_weight": qkv_weight, "out_weight": out_weight, "ln2_gain": ln2_gain, "ffn_in": ffn_in, "ffn_out": ffn_out, "expert_ids": expert_ids, "expert_in": expert_in, "expert_out": expert_out}


def layer_norm(row_data, gain_vector):
    row_data = row_data.astype(jnp.float32)
    centered = row_data - lax.optimization_barrier(jnp.mean(row_data, axis=-1, keepdims=True))
    spread = lax.optimization_barrier(jnp.mean(centered * centered, axis=-1, keepdims=True))
    return centered * lax.rsqrt(spread + 1e-06) * gain_vector

def attend_head(queries, key_rows, value_rows):
    scores = jnp.dot(queries, key_rows.T, preferred_element_type=jnp.float32) * DH ** (-0.5)
    row_max = lax.optimization_barrier(jnp.max(scores, axis=-1, keepdims=True))
    weights = jnp.exp(scores - row_max)
    probabilities = (weights / lax.optimization_barrier(jnp.sum(weights, axis=-1, keepdims=True))).astype(jnp.bfloat16)
    return jnp.dot(probabilities, value_rows, preferred_element_type=jnp.float32).astype(jnp.bfloat16)

def image_block(image_rows, ln1_gain, qkv_weight, out_weight, ln2_gain, ffn_in, ffn_out):
    normed = layer_norm(image_rows, ln1_gain).astype(jnp.bfloat16)
    projected = jnp.dot(normed, qkv_weight.reshape(D, HEADS * 3 * DH), preferred_element_type=jnp.float32)
    projected = projected.astype(jnp.bfloat16).reshape(SEQ, HEADS, 3, DH)
    by_head = jnp.transpose(projected, (1, 2, 0, 3))
    attended = lax.map(lambda head_item: attend_head(head_item[0], head_item[1], head_item[2]), by_head)
    attended = jnp.transpose(attended, (1, 0, 2)).reshape(SEQ, HEADS * DH)
    mixed_heads = jnp.dot(attended, out_weight, preferred_element_type=jnp.float32)
    hidden_state = (image_rows.astype(jnp.float32) + mixed_heads).astype(jnp.bfloat16)
    normed_two = layer_norm(hidden_state, ln2_gain).astype(jnp.bfloat16)
    inner_sum = jnp.dot(normed_two, ffn_in, preferred_element_type=jnp.float32)
    hidden_units = jax.nn.gelu(inner_sum, approximate=False).astype(jnp.bfloat16)
    dense_sum = jnp.zeros((SEQ, D), jnp.float32)
    for column_block in range(N_COL):
        lower_edge = column_block * FF_BLOCK
        part_sum = jnp.dot(hidden_units[:, lower_edge:lower_edge + FF_BLOCK], ffn_out[lower_edge:lower_edge + FF_BLOCK], preferred_element_type=jnp.float32)
        rounded = lax.optimization_barrier(part_sum.astype(jnp.bfloat16))
        dense_sum = dense_sum + rounded.astype(jnp.float32)
    return (hidden_state, normed_two, dense_sum)

def reference(tokens, ln1_gain, qkv_weight, out_weight, ln2_gain, ffn_in, ffn_out, expert_ids, expert_in, expert_out):
    device_count = N_ROW * N_COL
    images = tokens.reshape(TOKENS // SEQ, SEQ, D)

    def one_image(image_rows):
        return image_block(image_rows, ln1_gain, qkv_weight, out_weight, ln2_gain, ffn_in, ffn_out)
    hidden_state, normed_two, dense_sum = lax.map(one_image, images)
    hidden_state = hidden_state.reshape(TOKENS, D)
    normed_two = normed_two.reshape(TOKENS, D)
    dense_sum = dense_sum.reshape(TOKENS, D)
    chosen = expert_ids[:, 0].astype(jnp.int32)
    by_device = chosen.reshape(device_count, TOK_DEV)
    one_hot = (by_device[:, :, None] == jnp.arange(EXPERTS, dtype=jnp.int32)[None, None, :]).astype(jnp.int32)
    earlier = jnp.cumsum(one_hot, axis=1) - one_hot
    local_slot = lax.optimization_barrier(jnp.sum(earlier * one_hot, axis=2))
    global_slot = (local_slot + CAP * jnp.arange(device_count, dtype=jnp.int32)[:, None]).reshape(TOKENS).astype(jnp.int32)
    buffers = jnp.zeros((EXPERTS, device_count * CAP, D), normed_two.dtype).at[chosen, global_slot].set(normed_two)
    paired_in = expert_in.reshape(EXPERTS, 2, D, HALF)
    paired_out = expert_out.reshape(EXPERTS, 2, HALF, D)

    def run_expert(operands):
        buffer_rows, weights_in, weights_out = operands
        whole_in = jnp.concatenate((weights_in[0], weights_in[1]), axis=1)
        whole_out = jnp.concatenate((weights_out[0], weights_out[1]), axis=0)
        inner_units = jax.nn.gelu(jnp.dot(buffer_rows, whole_in, preferred_element_type=jnp.float32), approximate=False).astype(jnp.bfloat16)
        return jnp.dot(inner_units, whole_out, preferred_element_type=jnp.float32).astype(jnp.bfloat16)
    results = lax.map(run_expert, (buffers, paired_in, paired_out))
    expert_rows = results[chosen, global_slot]
    block_out = hidden_state.astype(jnp.float32) + dense_sum + expert_rows.astype(jnp.float32)
    return block_out.astype(jnp.bfloat16)
```

```python
import functools
import jax
import jax.numpy as jnp
from jax import lax
from jax.experimental import pallas as pl
from jax.experimental.pallas import tpu as pltpu
from jax.sharding import PartitionSpec as P

MESH = pl.DeviceIdType.MESH


def flipped(index, bit):
    return index + bit - 2 * bit * ((index // bit) % 2)


def comm_body(plan, row_total, col_total, *refs):
    gathers, spreads, sums, shuffles, units = plan
    count = len(gathers) + len(spreads) + len(sums) + len(shuffles)
    ins, refs = refs[:count], refs[count:]
    operands, refs = refs[: 2 * len(units)], refs[2 * len(units) :]
    outs, refs = refs[:count], refs[count:]
    results, refs = refs[: len(units)], refs[len(units) :]
    stages, refs = refs[:count], refs[count:]
    sum_slots = refs[: 2 * len(sums)]
    send, recv, local = refs[2 * len(sums) :]
    row = lax.axis_index("row")
    col = lax.axis_index("col")

    barrier = pltpu.get_barrier_semaphore()
    peers = 0
    if gathers or shuffles:
        for step in range(1, row_total):
            pl.semaphore_signal(
                barrier, inc=1, device_id=(lax.rem(row + step, row_total), col), device_id_type=MESH
            )
            peers += 1
    if spreads or sums:
        for step in range(1, col_total):
            pl.semaphore_signal(
                barrier, inc=1, device_id=(row, lax.rem(col + step, col_total)), device_id_type=MESH
            )
            peers += 1

    loads = []
    for i in range(count):
        load = pltpu.make_async_copy(ins[i], stages[i], local.at[i])
        load.start()
        loads.append(load)
    pl.semaphore_wait(barrier, peers)

    serial = [0]
    finish = []
    pending = []
    kept = []

    def number():
        serial[0] += 1
        return serial[0] - 1

    def remote(k, src, dst, device):
        return pltpu.make_async_remote_copy(
            src, dst, send.at[k], recv.at[k], device_id=device, device_id_type=MESH
        )

    def copy(src, dst, arriving, device):
        k = number()
        out = remote(k, src, dst, device)
        out.start()
        finish.append((None, out))
        return remote(k, src, arriving, device)

    def copy_if(condition, k, src, dst, device):
        out = remote(k, src, dst, device)
        pl.when(condition)(out.start)
        finish.append((condition, out))

    def keep(i, src, dst):
        own = pltpu.make_async_copy(src, dst, local.at[count + i])
        own.start()
        kept.append(own)

    right = (row, lax.rem(col + 1, col_total))
    left = (row, lax.rem(col + col_total - 1, col_total))
    last = col_total - 1
    lines = []
    base = len(gathers)
    for i in range(base, base + len(spreads)):
        loads[i].wait()
        size = ins[i].shape[0]

        def block(index, i=i, size=size):
            index = lax.rem(index + col_total, col_total)
            return outs[i].at[pl.ds(pl.multiple_of(index * size, size), size)]

        keys = [(number(), number()) for _ in range(last)]
        copy_if(col < last, keys[0][0], stages[i], block(col), right)
        copy_if(col > 0, keys[0][1], stages[i], block(col), left)
        keep(i, stages[i], block(col))

        def advance(step, block=block, keys=keys):
            got = block(col - 1 - step)
            pl.when(col > step)(remote(keys[step][0], got, got, right).wait_recv)
            if step + 1 < last:
                copy_if((col > step) & (col < last), keys[step + 1][0], got, got, right)
            got = block(col + 1 + step)
            pl.when(col + step < last)(remote(keys[step][1], got, got, left).wait_recv)
            if step + 1 < last:
                copy_if((col + step < last) & (col > 0), keys[step + 1][1], got, got, left)

        lines.append(advance)
    base += len(spreads)
    for j in range(len(sums)):
        i = base + j
        loads[i].wait()
        stage, total = stages[i], outs[i]
        slots, merged = sum_slots[2 * j], sum_slots[2 * j + 1]
        keys = [number() for _ in range(col_total)]
        merge = col_total >= 4
        if merge:
            key = number()
            copy_if(col == 0, key, stage.at[last], merged, right)
            copy_if(col == last, key, stage.at[0], merged, left)

        def send_block(target, condition, source, stage=stage, slots=slots, keys=keys):
            out = pltpu.make_async_remote_copy(
                source,
                slots.at[col],
                send.at[keys[target]],
                recv.at[keys[0] + col],
                device_id=(row, target),
                device_id_type=MESH,
            )
            pl.when(condition)(out.start)
            finish.append((condition, out))

        for target in range(col_total):
            condition = col != target
            if merge and target == last:
                condition = condition & (col > 1)
            if merge and target == 0:
                condition = condition & (col < last - 1)
            send_block(target, condition, stage.at[target])
        total[...] = stage[pl.ds(col, 1)][0].astype(jnp.float32)

        def combine(stage=stage, merged=merged, key=key if merge else 0, send_block=send_block):
            for target, holder in ((last, 1), (0, last - 1)):
                pl.when(col == holder)(remote(key, merged, merged, right).wait_recv)

                @pl.when(col == holder)
                def _():
                    merged[...] = (
                        merged[...].astype(jnp.float32) + stage[target].astype(jnp.float32)
                    ).astype(merged.dtype)

                send_block(target, col == holder, merged)

        def collect(total=total, slots=slots, keys=keys, merge=merge):
            for source in range(col_total):
                condition = col != source
                if merge and source == 0:
                    condition = condition & (col < last)
                if merge and source == last:
                    condition = condition & (col > 0)
                slot = slots.at[source]
                pl.when(condition)(remote(keys[source], slot, slot, right).wait_recv)

                @pl.when(condition)
                def _():
                    total[...] += slots[source].astype(jnp.float32)

        def advance(step, combine=combine, collect=collect, merge=merge):
            if step == 0 and merge:
                combine()
            if step == last - 1:
                collect()

        lines.append(advance)
    base += len(sums)
    for i in range(base, base + len(shuffles)):
        loads[i].wait()
        for step in range(1, row_total):
            to = lax.rem(row + (step if shuffles[i - base] > 0 else row_total - step), row_total)
            slot = outs[i].at[step]
            pending.append(copy(stages[i].at[step], slot, slot, (to, col)))
        keep(i, stages[i].at[0], outs[i].at[0])

    partner = flipped(row, 1)
    relay = row_total == 8

    def piece(i, index, half):
        depth, width = ins[i].shape
        start, size = (0, depth) if half is None else (half * (depth // 2), depth // 2)
        if gathers[i] == 0:
            return outs[i].at[pl.ds(pl.multiple_of(index * depth + start, size), size)]
        return outs[i].at[pl.ds(start, size), pl.ds(pl.multiple_of(index * width, width), width)]

    arrivals = []
    for i in range(len(gathers)):
        loads[i].wait()
        mine = piece(i, row, None)
        if relay:
            sources = [flipped(row, 2), flipped(row, 4)]
            targets = sources
        else:
            sources = [lax.rem(row + row_total - 2 * d, row_total) for d in range(1, row_total // 2)]
            targets = [lax.rem(row + 2 * d, row_total) for d in range(1, row_total // 2)]
        first = [
            (source, copy(stages[i], mine, piece(i, source, None), (target, col)))
            for source, target in zip(sources, targets)
        ]
        pending.append(copy(stages[i], mine, piece(i, partner, None), (partner, col)))
        keep(i, stages[i], mine)
        arrivals.append(first)

    def hand_on(i, source, half):
        got = piece(i, source, half)
        pending.append(copy(got, got, piece(i, flipped(source, 1), half), (partner, col)))

    seconds = []

    def first_level(i):
        if not relay:
            for source, arrival in arrivals[i]:
                arrival.wait_recv()
                hand_on(i, source, None)
            return
        (by_x, from_x), (by_y, from_y) = arrivals[i]
        across = flipped(by_x, 4)
        from_x.wait_recv()
        got = piece(i, by_x, 0)
        diag_a = copy(got, got, piece(i, across, 0), (by_y, col))
        hand_on(i, by_x, None)
        from_y.wait_recv()
        got = piece(i, by_y, 1)
        diag_b = copy(got, got, piece(i, across, 1), (by_x, col))
        hand_on(i, by_y, None)
        seconds.append((i, across, diag_a, diag_b))

    early = len(gathers) // 2 if lines else 0
    for step in range(last if lines else 0):
        for advance in lines:
            advance(step)
        if step == 0:
            for i in range(early):
                first_level(i)
        if step == min(1, last - 1):
            for i in range(early, len(gathers)):
                first_level(i)
    if not lines:
        for i in range(len(gathers)):
            first_level(i)
    for n in range(len(units)):
        x_ref, w_ref, o_ref = operands[2 * n], operands[2 * n + 1], results[n]
        rows, depth = x_ref.shape
        width = w_ref.shape[1]
        tile = min(width, 256)
        pltpu.emit_pipeline(
            up_body if units[n] else plain_body,
            grid=(width // tile,),
            in_specs=[
                pl.BlockSpec((rows, depth), lambda j: (0, 0)),
                pl.BlockSpec((depth, tile), lambda j: (0, j)),
            ],
            out_specs=[pl.BlockSpec((rows, tile), lambda j: (0, j))],
        )(x_ref, w_ref, o_ref)
    for i, across, diag_a, diag_b in seconds:
        for half, arrival in ((0, diag_a), (1, diag_b)):
            arrival.wait_recv()
            hand_on(i, across, half)
    for arrival in pending:
        arrival.wait_recv()
    for condition, out in finish:
        if condition is None:
            out.wait_send()
        else:
            pl.when(condition)(out.wait_send)
    for own in kept:
        own.wait()


def exchange(name, collective_id, gathers=(), spreads=(), sums=(), shuffles=(), units=()):
    row_total = lax.axis_size("row")
    col_total = lax.axis_size("col")
    arrays, shapes, copies = [], [], 0
    hbm, vmem = pl.BlockSpec(memory_space=pl.ANY), pl.BlockSpec(memory_space=pltpu.VMEM)
    for array, axis in gathers:
        depth, width = array.shape
        arrays.append(array)
        shape = (depth * row_total, width) if axis == 0 else (depth, width * row_total)
        shapes.append((shape, array.dtype, hbm))
        copies += 9 if row_total == 8 else row_total
    for array in spreads:
        arrays.append(array)
        shape = (array.shape[0] * col_total,) + array.shape[1:]
        shapes.append((shape, array.dtype, hbm))
        copies += 2 * (col_total - 1)
    slots = []
    for array in sums:
        arrays.append(array)
        shapes.append((array.shape[1:], jnp.float32, vmem))
        slots += [pltpu.VMEM(array.shape, array.dtype), pltpu.VMEM(array.shape[1:], array.dtype)]
        copies += col_total + 1
    for array, _ in shuffles:
        arrays.append(array)
        shapes.append((array.shape, array.dtype, hbm))
        copies += row_total - 1
    operands = []
    for x, w, _ in units:
        operands += [x, w]
        shapes.append(((x.shape[0], w.shape[1]), jnp.bfloat16, hbm))
    plan = (
        [axis for _, axis in gathers],
        [0] * len(spreads),
        [0] * len(sums),
        [sign for _, sign in shuffles],
        [with_gelu for _, _, with_gelu in units],
    )
    return pl.pallas_call(
        functools.partial(comm_body, plan, row_total, col_total),
        out_shape=[jax.ShapeDtypeStruct(shape, dtype) for shape, dtype, _ in shapes],
        in_specs=[hbm] * (len(arrays) + len(operands)),
        out_specs=[spec for _, _, spec in shapes],
        scratch_shapes=[pltpu.VMEM(a.shape, a.dtype) for a in arrays]
        + slots
        + [
            pltpu.SemaphoreType.DMA((copies,)),
            pltpu.SemaphoreType.DMA((copies,)),
            pltpu.SemaphoreType.DMA((2 * len(arrays),)),
        ],
        compiler_params=pltpu.CompilerParams(
            collective_id=collective_id, has_side_effects=True, vmem_limit_bytes=16 * 2**20
        ),
        name=name,
    )(*arrays, *operands)


def plain_body(x_ref, w_ref, o_ref):
    inner = jnp.dot(x_ref[...], w_ref[...], preferred_element_type=jnp.float32)
    o_ref[...] = inner.astype(o_ref.dtype)


def up_body(x_ref, w_ref, o_ref):
    inner = jnp.dot(x_ref[...], w_ref[...], preferred_element_type=jnp.float32)
    o_ref[...] = (inner * (1.0 + lax.erf(inner * (0.5**0.5))) * 0.5).astype(o_ref.dtype)


def up_gelu(x, w):
    rows, depth = x.shape
    width = w.shape[1]
    tile = min(width, 256)
    return pl.pallas_call(
        up_body,
        grid=(width // tile,),
        out_shape=jax.ShapeDtypeStruct((rows, width), jnp.bfloat16),
        in_specs=[
            pl.BlockSpec((rows, depth), lambda j: (0, 0)),
            pl.BlockSpec((depth, tile), lambda j: (0, j)),
        ],
        out_specs=pl.BlockSpec((rows, tile), lambda j: (0, j)),
        compiler_params=pltpu.CompilerParams(vmem_limit_bytes=32 * 2**20),
        cost_estimate=pl.CostEstimate(
            flops=2 * rows * depth * width,
            bytes_accessed=2 * (rows * depth + depth * width + rows * width),
            transcendentals=0,
        ),
        name="up_gelu",
    )(x, w)


def layer_norm(row_data, gain_vector):
    row_data = row_data.astype(jnp.float32)
    centered = row_data - jnp.mean(row_data, axis=-1, keepdims=True)
    spread = jnp.mean(centered * centered, axis=-1, keepdims=True)
    return centered * lax.rsqrt(spread + 1e-06) * gain_vector


def matmul(a, b):
    return jnp.dot(a, b, preferred_element_type=jnp.float32)


def chosen(table, index):
    value = jnp.int32(table[0])
    for n in range(1, len(table)):
        value = jnp.where(index == n, jnp.int32(table[n]), value)
    return value


def near_first(total):
    return [sorted(range(total), key=lambda b: (abs(b - c), b)) for c in range(total)]


def far_first(total):
    return [sorted(range(total), key=lambda b: (-abs(b - c), -b)) for c in range(total)]


def block_body(sizes, *refs):
    row_total, col_total, capacity, heads, parts = sizes
    (tokens_in, gain_one, gain_two, ids_in, qkv_in, out_in, up_in, down_in, first_in, second_in) = refs[:10]
    result = refs[10]
    (tokens, image, fresh, qkv, outw, upw, downw, first, second, proj, attended, stage, slots) = refs[11:24]
    (own_sum, hidden, table, landed, returned, units, codes) = refs[24:31]
    (load_sem, ag_send, ag_recv, code_send, code_recv, rs_send, rs_recv) = refs[31:38]
    (gather_send, gather_recv, out_send, out_recv, back_send, back_recv) = refs[38:]
    row = lax.axis_index("row")
    col = lax.axis_index("col")
    last = col_total - 1
    tok, model = tokens.shape
    size = tok // parts
    head_dim = attended.shape[1] // heads
    f32 = jnp.float32

    barrier = pltpu.get_barrier_semaphore()
    for step in range(1, row_total):
        pl.semaphore_signal(
            barrier, inc=1, device_id=(lax.rem(row + step, row_total), col), device_id_type=MESH
        )
    for step in range(1, col_total):
        pl.semaphore_signal(
            barrier, inc=1, device_id=(row, lax.rem(col + step, col_total)), device_id_type=MESH
        )

    finish = []

    def remote(src, dst, send, recv, device):
        return pltpu.make_async_remote_copy(
            src, dst, send, recv, device_id=device, device_id_type=MESH
        )

    def launch(copy, condition=None, into=None):
        if condition is None:
            copy.start()
        else:
            pl.when(condition)(copy.start)
        (finish if into is None else into).append((condition, copy))

    def drain(items):
        for condition, copy in items:
            if condition is None:
                copy.wait_send()
            else:
                pl.when(condition)(copy.wait_send)
        items.clear()

    wholes = [(qkv, qkv_in, 0), (outw, out_in, 1), (upw, up_in, 0), (downw, down_in, 1)]

    def piece(g, index, half=None):
        whole, part, axis = wholes[g]
        depth, width = part.shape
        start, count = (0, depth) if half is None else (half * (depth // 2), depth // 2)
        if axis == 0:
            return whole.at[pl.ds(pl.multiple_of(index * depth + start, count), count)]
        return whole.at[pl.ds(start, count), pl.ds(pl.multiple_of(index * width, width), width)]

    loads = [pltpu.make_async_copy(tokens_in, tokens, load_sem.at[0])]
    for g in range(4):
        loads.append(pltpu.make_async_copy(wholes[g][1], piece(g, row), load_sem.at[1 + g]))
    loads.append(pltpu.make_async_copy(first_in, first, load_sem.at[5]))
    loads.append(pltpu.make_async_copy(second_in, second, load_sem.at[6]))
    for load in loads:
        load.start()

    partner, by_x, by_y = flipped(row, 1), flipped(row, 2), flipped(row, 4)
    across = flipped(by_x, 4)

    def gather_copy(g, key, index, half, target):
        part = piece(g, index, half)
        return remote(part, part, gather_send.at[g, key], gather_recv.at[g, key], (target, col))

    def gather_wait(g, key, index, half=None):
        gather_copy(g, key, index, half, partner).wait_recv()

    def gather_start(g):
        loads[1 + g].wait()
        launch(gather_copy(g, 0, row, None, by_x))
        launch(gather_copy(g, 1, row, None, by_y))
        launch(gather_copy(g, 2, row, None, partner))

    def gather_relay(g):
        gather_wait(g, 0, by_x)
        launch(gather_copy(g, 3, by_x, 0, by_y))
        launch(gather_copy(g, 5, by_x, None, partner))
        gather_wait(g, 1, by_y)
        launch(gather_copy(g, 4, by_y, 1, by_x))
        launch(gather_copy(g, 6, by_y, None, partner))

    def gather_finish(g):
        gather_wait(g, 3, across, 0)
        launch(gather_copy(g, 7, across, 0, partner))
        gather_wait(g, 4, across, 1)
        launch(gather_copy(g, 8, across, 1, partner))

    def gather_complete(g):
        gather_wait(g, 2, partner)
        gather_wait(g, 5, flipped(by_x, 1))
        gather_wait(g, 6, flipped(by_y, 1))
        gather_wait(g, 7, flipped(across, 1), 0)
        gather_wait(g, 8, flipped(across, 1), 1)

    near = [chosen([order[k] for order in near_first(col_total)], col) for k in range(col_total)]
    far = [chosen([order[k] for order in far_first(col_total)], col) for k in range(col_total)]

    def rows_of(h):
        return pl.ds(h * size, size)

    def spread_copy(phase, b, h, target, way):
        part = (image, fresh)[phase].at[b, rows_of(h)]
        return remote(
            part, part, ag_send.at[phase, b, h, way], ag_recv.at[phase, b, h], (row, target)
        )

    def spread_start(phase, h):
        launch(spread_copy(phase, col, h, lax.rem(col + 1, col_total), 0), col < last)
        launch(spread_copy(phase, col, h, lax.rem(col + last, col_total), 1), col > 0)

    def onward(b):
        return jnp.where(b < col, lax.rem(col + 1, col_total), lax.rem(col + last, col_total))

    def more(b):
        return jnp.where(b < col, col < last, col > 0)

    def spread_step(phase, b, h):
        copy = spread_copy(phase, b, h, onward(b), 0)
        copy.wait_recv()
        launch(copy, more(b))

    def code_copy(b, target, way):
        return remote(
            codes.at[b], codes.at[b], code_send.at[b, way], code_recv.at[b], (row, target)
        )

    def sum_copy(phase, b, h):
        side = jnp.where(b > col, 0, 1)
        target = jnp.where(b > col, lax.rem(col + 1, col_total), lax.rem(col + last, col_total))
        return remote(
            stage.at[b, rows_of(h)],
            slots.at[side, b, rows_of(h)],
            rs_send.at[phase, b, h],
            rs_recv.at[phase, side, b, h],
            (row, target),
        )

    def fed(b):
        return jnp.where(b > col, col > 0, col < last)

    sums = []

    def sum_edge(phase, b, h):
        launch(sum_copy(phase, b, h), jnp.logical_not(fed(b)), sums)

    def sum_step(phase, b, h):
        copy = sum_copy(phase, b, h)

        @pl.when(fed(b))
        def _():
            side = jnp.where(b > col, 0, 1)
            copy.wait_recv()
            held = stage[b, rows_of(h)].astype(f32) + slots[side, b, rows_of(h)].astype(f32)
            stage[b, rows_of(h)] = held.astype(stage.dtype)

        launch(copy, fed(b), sums)

    def sum_own(phase, h):
        for side, condition in ((0, col > 0), (1, col < last)):

            @pl.when(condition)
            def _():
                slot = slots.at[side, col, rows_of(h)]
                remote(
                    slot, slot, rs_send.at[phase, col, h], rs_recv.at[phase, side, col, h], (row, onward(col))
                ).wait_recv()
                own_sum[rows_of(h)] += slots[side, col, rows_of(h)].astype(f32)

    def norm_rows(source, gain, target, index, h):
        for start in range(h * size, (h + 1) * size, 32):
            rows = pl.ds(start, 32)
            target[index, rows] = layer_norm(source[rows], gain[...]).astype(target.dtype)

    def columns(width, tile, body):
        def step(j, carry):
            body(pl.ds(pl.multiple_of(j * tile, tile), tile))
            return carry

        lax.fori_loop(0, width // tile, step, 0)

    loads[0].wait()
    norm_rows(tokens, gain_one, image, col, 0)

    named = jnp.broadcast_to(ids_in[...], (tok, tok)).astype(f32)
    across_ids = named.T
    earlier = lax.broadcasted_iota(jnp.int32, (tok, tok), 0) < lax.broadcasted_iota(
        jnp.int32, (tok, tok), 1
    )
    rank = jnp.sum(jnp.where(earlier & (named == across_ids), 1.0, 0.0), axis=0, keepdims=True)
    code = across_ids[0:8] * capacity + rank
    codes[col] = code.astype(jnp.int32)

    pl.semaphore_wait(barrier, row_total + col_total - 2)
    spread_start(0, 0)
    gather_start(0)
    for h in range(1, parts):
        norm_rows(tokens, gain_one, image, col, h)
        spread_start(0, h)
    launch(code_copy(col, lax.rem(col + 1, col_total), 0), col < last)
    launch(code_copy(col, lax.rem(col + last, col_total), 1), col > 0)
    gather_start(1)

    def project(b):
        def tile(at):
            inner = matmul(image[b], qkv[:, at])
            proj[pl.ds(pl.multiple_of(b * tok, tok), tok), at] = inner.astype(proj.dtype)

        columns(qkv.shape[1], 512, tile)

    def arrive(phase, k):
        for h in range(parts):
            spread_step(phase, near[k], h)

    def arrive_code(k):
        copy = code_copy(near[k], onward(near[k]), 0)
        copy.wait_recv()
        launch(copy, more(near[k]))

    arrive(0, 1)
    arrive_code(1)
    gather_relay(0)
    for k in range(2, col_total - 1):
        arrive(0, k)
        arrive_code(k)
    gather_relay(1)
    gather_start(2)
    gather_start(3)
    gather_finish(0)
    gather_finish(1)
    gather_complete(0)
    for k in range(col_total - 1):
        project(near[k])
    arrive(0, last)
    arrive_code(last)
    project(near[last])
    gather_complete(1)

    def attend(b):
        mine = pl.ds(pl.multiple_of(b * tok, tok), tok)
        for n in range(heads):
            base = 3 * n * head_dim
            query = proj[mine, base : base + head_dim]
            keys = proj[:, base + head_dim : base + 2 * head_dim]
            values = proj[:, base + 2 * head_dim : base + 3 * head_dim]
            scores = lax.dot_general(
                query, keys, (((1,), (1,)), ((), ())), preferred_element_type=f32
            )
            scores = scores * (head_dim ** (-0.5))
            weights = jnp.exp(scores - jnp.max(scores, axis=-1, keepdims=True))
            weights = weights / jnp.sum(weights, axis=-1, keepdims=True)
            attended[:, n * head_dim : (n + 1) * head_dim] = matmul(
                weights.astype(jnp.bfloat16), values
            ).astype(jnp.bfloat16)

    def head_terms(b, store):
        def tile(at):
            store(at, matmul(attended[...], outw[:, at]))

        columns(model, 512, tile)

    def to_stage(b):
        def store(at, inner):
            stage[b, :, at] = inner.astype(stage.dtype)

        return store

    def to_own(at, inner):
        own_sum[:, at] = inner

    for k in range(last):
        attend(far[k])
        head_terms(far[k], to_stage(far[k]))
        sum_edge(0, far[k], 0)
    for h in range(1, parts):
        for k in range(last):
            sum_edge(0, far[k], h)
    attend(col)
    head_terms(col, to_own)

    def placing(b):
        slot = lax.broadcasted_iota(jnp.int32, (row_total * capacity, tok), 0)
        wanted = slot + lax.div(col, 2) * capacity
        for n in range(1, row_total):
            wanted += jnp.where(slot >= n * capacity, (col_total // 2 - 1) * capacity, 0)
        return jnp.where(wanted == codes[b][0:1], 1.0, 0.0)

    def group(index):
        return pl.ds(pl.multiple_of(index * capacity, capacity), capacity)

    def out_copy(b, source, target):
        return remote(
            table.at[b, group(target)],
            landed.at[b, group(source)],
            out_send.at[b, target],
            out_recv.at[b, source],
            (target, col),
        )

    def back_copy(b, holder, target):
        return remote(
            landed.at[b, group(target)],
            returned.at[b, group(holder)],
            back_send.at[b, target],
            back_recv.at[b, holder],
            (target, col),
        )

    def dispatch(b):
        place = placing(b).astype(jnp.bfloat16)

        def tile(at):
            table[b, :, at] = matmul(place, fresh[b, :, at]).astype(table.dtype)

        columns(model, 512, tile)
        for flip in (2, 4, 6, 3, 5, 7, 1):
            launch(out_copy(b, row, lax.bitwise_xor(row, flip)))
        landed[b, group(row)] = table[b, group(row)]

    def with_gelu(inner):
        return (inner * (1.0 + lax.erf(inner * (0.5**0.5))) * 0.5).astype(jnp.bfloat16)

    def expert(b):
        for flip in range(1, row_total):
            other = lax.bitwise_xor(row, flip)
            out_copy(b, other, row).wait_recv()

        def up(at):
            units[:, at] = with_gelu(matmul(landed[b], first[:, at]))

        columns(first.shape[1], 512, up)

        def down(at):
            landed[b, :, at] = matmul(units[...], second[:, at]).astype(landed.dtype)

        columns(model, 512, down)
        for flip in (2, 4, 6, 3, 5, 7, 1):
            launch(back_copy(b, row, lax.bitwise_xor(row, flip)))
        returned[b, group(row)] = landed[b, group(row)]

    def dense(b, store):
        def up(at):
            units[:, at] = with_gelu(matmul(fresh[b], upw[:, at]))

        columns(upw.shape[1], 512, up)

        def down(at):
            store(at, matmul(units[...], downw[:, at]))

        columns(model, 512, down)

    def combine(b, own):
        for flip in range(1, row_total):
            other = lax.bitwise_xor(row, flip)
            back_copy(b, other, row).wait_recv()
        pick = placing(b).T.astype(jnp.bfloat16)

        def tile(at):
            inner = matmul(pick, returned[b, :, at])
            if own:
                own_sum[:, at] += inner
            else:
                stage[b, :, at] = (stage[b, :, at].astype(f32) + inner).astype(stage.dtype)

        columns(model, 512, tile)

    def close_hidden(h):
        sum_own(0, h)
        rows = rows_of(h)
        hidden[rows] = (tokens[rows].astype(f32) + own_sum[rows]).astype(hidden.dtype)
        norm_rows(hidden, gain_two, fresh, col, h)
        spread_start(1, h)

    for k in range(last):
        sum_step(0, far[k], 0)
    close_hidden(0)
    gather_relay(2)
    for h in range(1, parts):
        for k in range(last):
            sum_step(0, far[k], h)
            spread_step(1, near[k + 1], h - 1)
        close_hidden(h)
        if h == 1:
            gather_relay(3)
    gather_finish(2)
    dispatch(col)
    for k in range(1, col_total):
        spread_step(1, near[k], parts - 1)
        dispatch(near[k])
        if k == 1:
            gather_finish(3)
    drain(sums)
    loads[5].wait()
    loads[6].wait()
    expert(near[0])
    gather_complete(2)
    gather_complete(3)
    for k in range(1, col_total):
        expert(near[k])
        dense(near[k], to_stage(near[k]))
    dense(col, to_own)
    for k in range(1, col_total):
        combine(near[k], False)
        for h in range(parts):
            sum_edge(1, near[k], h)
    combine(col, True)
    for h in range(parts):
        for k in range(last):
            sum_step(1, far[k], h)
    for h in range(parts):
        sum_own(1, h)
        rows = rows_of(h)
        result[rows] = (hidden[rows].astype(f32) + own_sum[rows]).astype(result.dtype)
    drain(sums)
    drain(finish)


def fused_block(tokens, gain_one, qkv_part, out_part, gain_two, up_part, down_part, ids, first, second, capacity, heads):
    row_total = lax.axis_size("row")
    col_total = lax.axis_size("col")
    tok, model = tokens.shape
    parts = 2
    hbm, vmem = pl.BlockSpec(memory_space=pl.ANY), pl.BlockSpec(memory_space=pltpu.VMEM)
    bf16 = jnp.bfloat16
    three = qkv_part.shape[1]
    width = out_part.shape[0]
    slot_count = row_total * capacity
    dma = pltpu.SemaphoreType.DMA
    scratch = [
        pltpu.VMEM((tok, model), bf16),
        pltpu.VMEM((col_total, tok, model), bf16),
        pltpu.VMEM((col_total, tok, model), bf16),
        pltpu.VMEM((row_total * qkv_part.shape[0], three), bf16),
        pltpu.VMEM((width, row_total * out_part.shape[1]), bf16),
        pltpu.VMEM((row_total * up_part.shape[0], up_part.shape[1]), bf16),
        pltpu.VMEM((down_part.shape[0], row_total * down_part.shape[1]), bf16),
        pltpu.VMEM(first.shape, bf16),
        pltpu.VMEM(second.shape, bf16),
        pltpu.VMEM((col_total * tok, three), bf16),
        pltpu.VMEM((tok, width), bf16),
        pltpu.VMEM((col_total, tok, model), bf16),
        pltpu.VMEM((2, col_total, tok, model), bf16),
        pltpu.VMEM((tok, model), jnp.float32),
        pltpu.VMEM((tok, model), bf16),
        pltpu.VMEM((col_total, slot_count, model), bf16),
        pltpu.VMEM((col_total, slot_count, model), bf16),
        pltpu.VMEM((col_total, slot_count, model), bf16),
        pltpu.VMEM((tok, max(up_part.shape[1], first.shape[1])), bf16),
        pltpu.VMEM((col_total, 8, tok), jnp.int32),
        dma((7,)),
        dma((2, col_total, parts, 2)),
        dma((2, col_total, parts)),
        dma((col_total, 2)),
        dma((col_total,)),
        dma((2, col_total, parts)),
        dma((2, 2, col_total, parts)),
        dma((4, 9)),
        dma((4, 9)),
        dma((col_total, row_total)),
        dma((col_total, row_total)),
        dma((col_total, row_total)),
        dma((col_total, row_total)),
    ]
    return pl.pallas_call(
        functools.partial(block_body, (row_total, col_total, capacity, heads, parts)),
        out_shape=jax.ShapeDtypeStruct((tok, model), bf16),
        in_specs=[hbm, vmem, vmem, vmem] + [hbm] * 6,
        out_specs=vmem,
        scratch_shapes=scratch,
        compiler_params=pltpu.CompilerParams(
            collective_id=0, has_side_effects=True, vmem_limit_bytes=67043328
        ),
        name="block",
    )(
        tokens,
        gain_one.reshape(1, model),
        gain_two.reshape(1, model),
        ids,
        qkv_part,
        out_part,
        up_part,
        down_part,
        first,
        second,
    )


def shards(
    tokens,
    ln1_gain,
    qkv_weight,
    out_weight,
    ln2_gain,
    ffn_in,
    ffn_out,
    expert_ids,
    expert_in,
    expert_out,
):
    tok_count, model_width = tokens.shape
    row_total = lax.axis_size("row")
    col_total = lax.axis_size("col")
    row_index = lax.axis_index("row")
    col_index = lax.axis_index("col")
    expert_count = row_total * col_total // 2
    capacity = max(2, 2 * tok_count // expert_count)
    head_count, head_dim = qkv_weight.shape[1], qkv_weight.shape[3]
    seq_len = tok_count * col_total
    if row_total == 8 and col_total % 2 == 0 and capacity % 16 == 0:
        return fused_block(
            tokens,
            ln1_gain,
            qkv_weight.reshape(qkv_weight.shape[0], -1),
            out_weight,
            ln2_gain,
            ffn_in,
            ffn_out,
            expert_ids,
            expert_in[0],
            expert_out[0],
            capacity,
            head_count,
        )

    ids_block = jnp.broadcast_to(expert_ids[:, 0][None, :], (8, tok_count))
    qkv_whole, out_whole, image_rows, ids_all = exchange(
        "enter",
        0,
        gathers=((qkv_weight.reshape(qkv_weight.shape[0], -1), 0), (out_weight, 1)),
        spreads=(tokens, ids_block),
    )
    normed = layer_norm(image_rows, ln1_gain).astype(jnp.bfloat16)
    projected = matmul(normed, qkv_whole).astype(jnp.bfloat16)
    projected = projected.reshape(seq_len, head_count, 3, head_dim)
    queries, keys, values = projected[:, :, 0], projected[:, :, 1], projected[:, :, 2]
    scores = jnp.einsum("qhd,khd->hqk", queries, keys, preferred_element_type=jnp.float32)
    scores = scores * (head_dim ** (-0.5))
    weights = jnp.exp(scores - jnp.max(scores, axis=-1, keepdims=True))
    probabilities = (weights / jnp.sum(weights, axis=-1, keepdims=True)).astype(jnp.bfloat16)
    attended = jnp.einsum("hqk,khd->qhd", probabilities, values, preferred_element_type=jnp.float32)
    attended = attended.astype(jnp.bfloat16).reshape(seq_len, head_count * head_dim)
    head_terms = matmul(attended, out_whole).astype(jnp.bfloat16)
    head_terms = head_terms.reshape(col_total, tok_count, model_width)

    up_whole, mixed_heads = exchange("heads", 1, gathers=((ffn_in, 0),), sums=(head_terms,))
    hidden_mine = (tokens.astype(jnp.float32) + mixed_heads).astype(jnp.bfloat16)
    normed_mine = layer_norm(hidden_mine, ln2_gain).astype(jnp.bfloat16)

    down_whole, normed_image = exchange(
        "norms", 2, gathers=((ffn_out, 1),), spreads=(normed_mine,)
    )

    ids_rows = ids_all.reshape(col_total, 8, tok_count)[:, 0]
    expert_range = jnp.arange(expert_count, dtype=jnp.int32)
    one_hot = (ids_rows[:, :, None] == expert_range).astype(jnp.int32)
    earlier = jnp.cumsum(one_hot, axis=1) - one_hot
    slot_index = jnp.sum(earlier * one_hot, axis=2)
    block_index = jnp.arange(col_total, dtype=jnp.int32)[:, None]
    home_row = 2 * ids_rows // col_total
    mine = (2 * ids_rows % col_total) // 2 == col_index // 2
    step = (home_row - row_index + row_total) % row_total
    position = (step * col_total + block_index) * capacity + slot_index
    position = jnp.where(mine, position, -1).reshape(seq_len)
    slot_count = row_total * col_total * capacity
    slots = jnp.arange(slot_count, dtype=jnp.int32)
    placing = (slots[:, None] == position[None, :]).astype(jnp.bfloat16)
    picking = (position[:, None] == slots[None, :]).astype(jnp.bfloat16)

    table = matmul(placing, normed_image).astype(jnp.bfloat16)
    table = table.reshape(row_total, col_total * capacity, model_width)
    expert_rows, hidden_units = exchange(
        "dispatch", 3, shuffles=((table, 1),), units=((normed_image, up_whole, True),)
    )
    expert_units = up_gelu(expert_rows.reshape(slot_count, model_width), expert_in[0])
    partial_out = matmul(expert_units, expert_out[0]).astype(jnp.bfloat16)
    partial_out = partial_out.reshape(row_total, col_total * capacity, model_width)
    returned, dense_part = exchange(
        "collect", 4, shuffles=((partial_out, -1),), units=((hidden_units, down_whole, False),)
    )

    rows_two = returned.reshape(slot_count, model_width)
    partial = dense_part.astype(jnp.float32) + matmul(picking, rows_two)
    partial = partial.astype(jnp.bfloat16).reshape(col_total, tok_count, model_width)
    (total,) = exchange("leave", 5, sums=(partial,))
    return (hidden_mine.astype(jnp.float32) + total).astype(jnp.bfloat16)


def solution(mesh):
    in_specs = (
        P(("row", "col"), None),
        P(),
        P("row", "col", None, None),
        P("col", "row"),
        P(),
        P("row", "col"),
        P("col", "row"),
        P(("row", "col"), None),
        P(("row", "col"), None, None),
        P(("row", "col"), None, None),
    )
    out_specs = P(("row", "col"), None)
    return jax.shard_map(shards, mesh=mesh, in_specs=in_specs, out_specs=out_specs, check_vma=False)
```

```python
import functools
import jax
import jax.numpy as jnp
from jax import lax
from jax.experimental import pallas as pl
from jax.experimental.pallas import tpu as pltpu
from jax.sharding import PartitionSpec as P

MESH = pl.DeviceIdType.MESH


def flipped(index, bit):
    return index + bit - 2 * bit * ((index // bit) % 2)


def comm_body(plan, row_total, col_total, *refs):
    gathers, spreads, sums, shuffles, units = plan
    count = len(gathers) + len(spreads) + len(sums) + len(shuffles)
    ins, refs = refs[:count], refs[count:]
    operands, refs = refs[: 2 * len(units)], refs[2 * len(units) :]
    outs, refs = refs[:count], refs[count:]
    results, refs = refs[: len(units)], refs[len(units) :]
    stages, refs = refs[:count], refs[count:]
    sum_slots = refs[: 2 * len(sums)]
    send, recv, local = refs[2 * len(sums) :]
    row = lax.axis_index("row")
    col = lax.axis_index("col")

    barrier = pltpu.get_barrier_semaphore()
    peers = 0
    if gathers or shuffles:
        for step in range(1, row_total):
            pl.semaphore_signal(
                barrier, inc=1, device_id=(lax.rem(row + step, row_total), col), device_id_type=MESH
            )
            peers += 1
    if spreads or sums:
        for step in range(1, col_total):
            pl.semaphore_signal(
                barrier, inc=1, device_id=(row, lax.rem(col + step, col_total)), device_id_type=MESH
            )
            peers += 1

    loads = []
    for i in range(count):
        load = pltpu.make_async_copy(ins[i], stages[i], local.at[i])
        load.start()
        loads.append(load)
    pl.semaphore_wait(barrier, peers)

    serial = [0]
    finish = []
    pending = []
    kept = []

    def number():
        serial[0] += 1
        return serial[0] - 1

    def remote(k, src, dst, device):
        return pltpu.make_async_remote_copy(
            src, dst, send.at[k], recv.at[k], device_id=device, device_id_type=MESH
        )

    def copy(src, dst, arriving, device):
        k = number()
        out = remote(k, src, dst, device)
        out.start()
        finish.append((None, out))
        return remote(k, src, arriving, device)

    def copy_if(condition, k, src, dst, device):
        out = remote(k, src, dst, device)
        pl.when(condition)(out.start)
        finish.append((condition, out))

    def keep(i, src, dst):
        own = pltpu.make_async_copy(src, dst, local.at[count + i])
        own.start()
        kept.append(own)

    right = (row, lax.rem(col + 1, col_total))
    left = (row, lax.rem(col + col_total - 1, col_total))
    last = col_total - 1
    lines = []
    base = len(gathers)
    for i in range(base, base + len(spreads)):
        loads[i].wait()
        size = ins[i].shape[0]

        def block(index, i=i, size=size):
            index = lax.rem(index + col_total, col_total)
            return outs[i].at[pl.ds(pl.multiple_of(index * size, size), size)]

        keys = [(number(), number()) for _ in range(last)]
        copy_if(col < last, keys[0][0], stages[i], block(col), right)
        copy_if(col > 0, keys[0][1], stages[i], block(col), left)
        keep(i, stages[i], block(col))

        def advance(step, block=block, keys=keys):
            got = block(col - 1 - step)
            pl.when(col > step)(remote(keys[step][0], got, got, right).wait_recv)
            if step + 1 < last:
                copy_if((col > step) & (col < last), keys[step + 1][0], got, got, right)
            got = block(col + 1 + step)
            pl.when(col + step < last)(remote(keys[step][1], got, got, left).wait_recv)
            if step + 1 < last:
                copy_if((col + step < last) & (col > 0), keys[step + 1][1], got, got, left)

        lines.append(advance)
    base += len(spreads)
    for j in range(len(sums)):
        i = base + j
        loads[i].wait()
        stage, total = stages[i], outs[i]
        slots, merged = sum_slots[2 * j], sum_slots[2 * j + 1]
        keys = [number() for _ in range(col_total)]
        merge = col_total >= 4
        if merge:
            key = number()
            copy_if(col == 0, key, stage.at[last], merged, right)
            copy_if(col == last, key, stage.at[0], merged, left)

        def send_block(target, condition, source, stage=stage, slots=slots, keys=keys):
            out = pltpu.make_async_remote_copy(
                source,
                slots.at[col],
                send.at[keys[target]],
                recv.at[keys[0] + col],
                device_id=(row, target),
                device_id_type=MESH,
            )
            pl.when(condition)(out.start)
            finish.append((condition, out))

        for target in range(col_total):
            condition = col != target
            if merge and target == last:
                condition = condition & (col > 1)
            if merge and target == 0:
                condition = condition & (col < last - 1)
            send_block(target, condition, stage.at[target])
        total[...] = stage[pl.ds(col, 1)][0].astype(jnp.float32)

        def combine(stage=stage, merged=merged, key=key if merge else 0, send_block=send_block):
            for target, holder in ((last, 1), (0, last - 1)):
                pl.when(col == holder)(remote(key, merged, merged, right).wait_recv)

                @pl.when(col == holder)
                def _():
                    merged[...] = (
                        merged[...].astype(jnp.float32) + stage[target].astype(jnp.float32)
                    ).astype(merged.dtype)

                send_block(target, col == holder, merged)

        def collect(total=total, slots=slots, keys=keys, merge=merge):
            for source in range(col_total):
                condition = col != source
                if merge and source == 0:
                    condition = condition & (col < last)
                if merge and source == last:
                    condition = condition & (col > 0)
                slot = slots.at[source]
                pl.when(condition)(remote(keys[source], slot, slot, right).wait_recv)

                @pl.when(condition)
                def _():
                    total[...] += slots[source].astype(jnp.float32)

        def advance(step, combine=combine, collect=collect, merge=merge):
            if step == 0 and merge:
                combine()
            if step == last - 1:
                collect()

        lines.append(advance)
    base += len(sums)
    for i in range(base, base + len(shuffles)):
        loads[i].wait()
        for step in range(1, row_total):
            to = lax.rem(row + (step if shuffles[i - base] > 0 else row_total - step), row_total)
            slot = outs[i].at[step]
            pending.append(copy(stages[i].at[step], slot, slot, (to, col)))
        keep(i, stages[i].at[0], outs[i].at[0])

    partner = flipped(row, 1)
    relay = row_total == 8

    def piece(i, index, half):
        depth, width = ins[i].shape
        start, size = (0, depth) if half is None else (half * (depth // 2), depth // 2)
        if gathers[i] == 0:
            return outs[i].at[pl.ds(pl.multiple_of(index * depth + start, size), size)]
        return outs[i].at[pl.ds(start, size), pl.ds(pl.multiple_of(index * width, width), width)]

    arrivals = []
    for i in range(len(gathers)):
        loads[i].wait()
        mine = piece(i, row, None)
        if relay:
            sources = [flipped(row, 2), flipped(row, 4)]
            targets = sources
        else:
            sources = [lax.rem(row + row_total - 2 * d, row_total) for d in range(1, row_total // 2)]
            targets = [lax.rem(row + 2 * d, row_total) for d in range(1, row_total // 2)]
        first = [
            (source, copy(stages[i], mine, piece(i, source, None), (target, col)))
            for source, target in zip(sources, targets)
        ]
        pending.append(copy(stages[i], mine, piece(i, partner, None), (partner, col)))
        keep(i, stages[i], mine)
        arrivals.append(first)

    def hand_on(i, source, half):
        got = piece(i, source, half)
        pending.append(copy(got, got, piece(i, flipped(source, 1), half), (partner, col)))

    seconds = []

    def first_level(i):
        if not relay:
            for source, arrival in arrivals[i]:
                arrival.wait_recv()
                hand_on(i, source, None)
            return
        (by_x, from_x), (by_y, from_y) = arrivals[i]
        across = flipped(by_x, 4)
        from_x.wait_recv()
        got = piece(i, by_x, 0)
        diag_a = copy(got, got, piece(i, across, 0), (by_y, col))
        hand_on(i, by_x, None)
        from_y.wait_recv()
        got = piece(i, by_y, 1)
        diag_b = copy(got, got, piece(i, across, 1), (by_x, col))
        hand_on(i, by_y, None)
        seconds.append((i, across, diag_a, diag_b))

    early = len(gathers) // 2 if lines else 0
    for step in range(last if lines else 0):
        for advance in lines:
            advance(step)
        if step == 0:
            for i in range(early):
                first_level(i)
        if step == min(1, last - 1):
            for i in range(early, len(gathers)):
                first_level(i)
    if not lines:
        for i in range(len(gathers)):
            first_level(i)
    for n in range(len(units)):
        x_ref, w_ref, o_ref = operands[2 * n], operands[2 * n + 1], results[n]
        rows, depth = x_ref.shape
        width = w_ref.shape[1]
        tile = min(width, 256)
        pltpu.emit_pipeline(
            up_body if units[n] else plain_body,
            grid=(width // tile,),
            in_specs=[
                pl.BlockSpec((rows, depth), lambda j: (0, 0)),
                pl.BlockSpec((depth, tile), lambda j: (0, j)),
            ],
            out_specs=[pl.BlockSpec((rows, tile), lambda j: (0, j))],
        )(x_ref, w_ref, o_ref)
    for i, across, diag_a, diag_b in seconds:
        for half, arrival in ((0, diag_a), (1, diag_b)):
            arrival.wait_recv()
            hand_on(i, across, half)
    for arrival in pending:
        arrival.wait_recv()
    for condition, out in finish:
        if condition is None:
            out.wait_send()
        else:
            pl.when(condition)(out.wait_send)
    for own in kept:
        own.wait()


def exchange(name, collective_id, gathers=(), spreads=(), sums=(), shuffles=(), units=()):
    row_total = lax.axis_size("row")
    col_total = lax.axis_size("col")
    arrays, shapes, copies = [], [], 0
    hbm, vmem = pl.BlockSpec(memory_space=pl.ANY), pl.BlockSpec(memory_space=pltpu.VMEM)
    for array, axis in gathers:
        depth, width = array.shape
        arrays.append(array)
        shape = (depth * row_total, width) if axis == 0 else (depth, width * row_total)
        shapes.append((shape, array.dtype, hbm))
        copies += 9 if row_total == 8 else row_total
    for array in spreads:
        arrays.append(array)
        shape = (array.shape[0] * col_total,) + array.shape[1:]
        shapes.append((shape, array.dtype, hbm))
        copies += 2 * (col_total - 1)
    slots = []
    for array in sums:
        arrays.append(array)
        shapes.append((array.shape[1:], jnp.float32, vmem))
        slots += [pltpu.VMEM(array.shape, array.dtype), pltpu.VMEM(array.shape[1:], array.dtype)]
        copies += col_total + 1
    for array, _ in shuffles:
        arrays.append(array)
        shapes.append((array.shape, array.dtype, hbm))
        copies += row_total - 1
    operands = []
    for x, w, _ in units:
        operands += [x, w]
        shapes.append(((x.shape[0], w.shape[1]), jnp.bfloat16, hbm))
    plan = (
        [axis for _, axis in gathers],
        [0] * len(spreads),
        [0] * len(sums),
        [sign for _, sign in shuffles],
        [with_gelu for _, _, with_gelu in units],
    )
    return pl.pallas_call(
        functools.partial(comm_body, plan, row_total, col_total),
        out_shape=[jax.ShapeDtypeStruct(shape, dtype) for shape, dtype, _ in shapes],
        in_specs=[hbm] * (len(arrays) + len(operands)),
        out_specs=[spec for _, _, spec in shapes],
        scratch_shapes=[pltpu.VMEM(a.shape, a.dtype) for a in arrays]
        + slots
        + [
            pltpu.SemaphoreType.DMA((copies,)),
            pltpu.SemaphoreType.DMA((copies,)),
            pltpu.SemaphoreType.DMA((2 * len(arrays),)),
        ],
        compiler_params=pltpu.CompilerParams(
            collective_id=collective_id, has_side_effects=True, vmem_limit_bytes=16 * 2**20
        ),
        name=name,
    )(*arrays, *operands)


def plain_body(x_ref, w_ref, o_ref):
    inner = jnp.dot(x_ref[...], w_ref[...], preferred_element_type=jnp.float32)
    o_ref[...] = inner.astype(o_ref.dtype)


def up_body(x_ref, w_ref, o_ref):
    inner = jnp.dot(x_ref[...], w_ref[...], preferred_element_type=jnp.float32)
    o_ref[...] = (inner * (1.0 + lax.erf(inner * (0.5**0.5))) * 0.5).astype(o_ref.dtype)


def up_gelu(x, w):
    rows, depth = x.shape
    width = w.shape[1]
    tile = min(width, 256)
    return pl.pallas_call(
        up_body,
        grid=(width // tile,),
        out_shape=jax.ShapeDtypeStruct((rows, width), jnp.bfloat16),
        in_specs=[
            pl.BlockSpec((rows, depth), lambda j: (0, 0)),
            pl.BlockSpec((depth, tile), lambda j: (0, j)),
        ],
        out_specs=pl.BlockSpec((rows, tile), lambda j: (0, j)),
        compiler_params=pltpu.CompilerParams(vmem_limit_bytes=32 * 2**20),
        cost_estimate=pl.CostEstimate(
            flops=2 * rows * depth * width,
            bytes_accessed=2 * (rows * depth + depth * width + rows * width),
            transcendentals=0,
        ),
        name="up_gelu",
    )(x, w)


def layer_norm(row_data, gain_vector):
    row_data = row_data.astype(jnp.float32)
    centered = row_data - jnp.mean(row_data, axis=-1, keepdims=True)
    spread = jnp.mean(centered * centered, axis=-1, keepdims=True)
    return centered * lax.rsqrt(spread + 1e-06) * gain_vector


def matmul(a, b):
    return jnp.dot(a, b, preferred_element_type=jnp.float32)


def chosen(table, index):
    value = jnp.int32(table[0])
    for n in range(1, len(table)):
        value = jnp.where(index == n, jnp.int32(table[n]), value)
    return value


def near_first(total):
    return [sorted(range(total), key=lambda b: (abs(b - c), b)) for c in range(total)]


def far_first(total):
    last = total - 1
    return [
        sorted(range(total), key=lambda b: (-abs(b - c), c if b > c else last - c))
        for c in range(total)
    ]


def late_last(total):
    last = total - 1
    return [
        sorted(
            [b for b in range(total) if b != c],
            key=lambda b: b + c if b > c else 2 * last - b - c,
        )
        for c in range(total)
    ]


def block_body(sizes, *refs):
    row_total, col_total, capacity, heads, parts = sizes
    (tokens_in, gain_one, gain_two, ids_in, qkv_in, out_in, up_in, down_in, first_in, second_in) = refs[:10]
    result = refs[10]
    (tokens, image, fresh, qkv, outw, upw, downw, first, second, proj, attended, stage, slots) = refs[11:24]
    (own_sum, hidden, table, landed, returned, units, inner_units, codes) = refs[24:32]
    (load_sem, ag_send, ag_recv, code_send, code_recv, rs_send, rs_recv) = refs[32:39]
    (gather_send, gather_recv, out_send, out_recv, back_send, back_recv) = refs[39:]
    row = lax.axis_index("row")
    col = lax.axis_index("col")
    last = col_total - 1
    tok, model = tokens.shape
    size = tok // parts
    head_dim = attended.shape[1] // heads
    f32 = jnp.float32

    barrier = pltpu.get_barrier_semaphore()
    for step in range(1, row_total):
        pl.semaphore_signal(
            barrier, inc=1, device_id=(lax.rem(row + step, row_total), col), device_id_type=MESH
        )
    for step in range(1, col_total):
        pl.semaphore_signal(
            barrier, inc=1, device_id=(row, lax.rem(col + step, col_total)), device_id_type=MESH
        )

    finish = []

    def remote(src, dst, send, recv, device):
        return pltpu.make_async_remote_copy(
            src, dst, send, recv, device_id=device, device_id_type=MESH
        )

    def launch(copy, condition=None, into=None):
        if condition is None:
            copy.start()
        else:
            pl.when(condition)(copy.start)
        (finish if into is None else into).append((condition, copy))

    def drain(items):
        for condition, copy in items:
            if condition is None:
                copy.wait_send()
            else:
                pl.when(condition)(copy.wait_send)
        items.clear()

    cut = qkv_in.shape[0] // 2
    wholes = [
        (qkv, qkv_in, 0, 0, cut),
        (qkv, qkv_in, 0, cut, cut),
        (outw, out_in, 1, 0, out_in.shape[0]),
        (upw, up_in, 0, 0, up_in.shape[0]),
        (downw, down_in, 1, 0, down_in.shape[0] // 2),
        (downw, down_in, 1, down_in.shape[0] // 2, down_in.shape[0] // 2),
    ]

    def piece(g, index, half=None):
        whole, part, axis, start, count = wholes[g]
        depth, width = part.shape
        if half is not None:
            start, count = start + half * (count // 2), count // 2
        if axis == 0:
            return whole.at[pl.ds(pl.multiple_of(index * depth + start, count), count)]
        return whole.at[pl.ds(start, count), pl.ds(pl.multiple_of(index * width, width), width)]

    loads = [pltpu.make_async_copy(tokens_in, tokens, load_sem.at[0])]
    for g, (_, part, _, start, count) in enumerate(wholes):
        source = part.at[pl.ds(start, count)]
        loads.append(pltpu.make_async_copy(source, piece(g, row), load_sem.at[1 + g]))
    loads.append(pltpu.make_async_copy(first_in, first, load_sem.at[7]))
    loads.append(pltpu.make_async_copy(second_in, second, load_sem.at[8]))
    for load in loads:
        load.start()

    partner, by_x, by_y = flipped(row, 1), flipped(row, 2), flipped(row, 4)
    across = flipped(by_x, 4)

    def gather_copy(g, key, index, half, target):
        part = piece(g, index, half)
        return remote(part, part, gather_send.at[g, key], gather_recv.at[g, key], (target, col))

    def gather_wait(g, key, index, half=None):
        gather_copy(g, key, index, half, partner).wait_recv()

    def gather_start(g):
        loads[1 + g].wait()
        launch(gather_copy(g, 0, row, None, by_x))
        launch(gather_copy(g, 1, row, None, by_y))
        launch(gather_copy(g, 2, row, None, partner))

    def gather_relay(g):
        gather_wait(g, 0, by_x)
        launch(gather_copy(g, 3, by_x, 0, by_y))
        launch(gather_copy(g, 5, by_x, None, partner))
        gather_wait(g, 1, by_y)
        launch(gather_copy(g, 4, by_y, 1, by_x))
        launch(gather_copy(g, 6, by_y, None, partner))

    def gather_finish(g):
        gather_wait(g, 3, across, 0)
        launch(gather_copy(g, 7, across, 0, partner))
        gather_wait(g, 4, across, 1)
        launch(gather_copy(g, 8, across, 1, partner))

    def gather_complete(g):
        gather_wait(g, 2, partner)
        gather_wait(g, 5, flipped(by_x, 1))
        gather_wait(g, 6, flipped(by_y, 1))
        gather_wait(g, 7, flipped(across, 1), 0)
        gather_wait(g, 8, flipped(across, 1), 1)

    near = [chosen([order[k] for order in near_first(col_total)], col) for k in range(col_total)]
    late = [chosen([order[k] for order in late_last(col_total)], col) for k in range(last)]
    far = [chosen([order[k] for order in far_first(col_total)], col) for k in range(col_total)]

    def rows_of(h):
        return pl.ds(h * size, size)

    def spread_copy(phase, b, h, target, way):
        part = (image, fresh)[phase].at[b, rows_of(h)]
        return remote(
            part, part, ag_send.at[phase, b, h, way], ag_recv.at[phase, b, h], (row, target)
        )

    def spread_start(phase, h):
        launch(spread_copy(phase, col, h, lax.rem(col + 1, col_total), 0), col < last)
        launch(spread_copy(phase, col, h, lax.rem(col + last, col_total), 1), col > 0)

    def onward(b):
        return jnp.where(b < col, lax.rem(col + 1, col_total), lax.rem(col + last, col_total))

    def more(b):
        return jnp.where(b < col, col < last, col > 0)

    def spread_at(phase, distance, h):
        for other in (col - distance, col + distance):
            valid = (other >= 0) & (other <= last)
            b = lax.rem(other + col_total, col_total)
            copy = spread_copy(phase, b, h, onward(b), 0)
            pl.when(valid)(copy.wait_recv)
            launch(copy, valid & more(b))

    def code_copy(b, target, way):
        return remote(
            codes.at[b], codes.at[b], code_send.at[b, way], code_recv.at[b], (row, target)
        )

    def sum_copy(phase, b, h):
        side = jnp.where(b > col, 0, 1)
        target = jnp.where(b > col, lax.rem(col + 1, col_total), lax.rem(col + last, col_total))
        return remote(
            stage.at[b, rows_of(h)],
            slots.at[side, b, rows_of(h)],
            rs_send.at[phase, b, h],
            rs_recv.at[phase, side, b, h],
            (row, target),
        )

    def fed(b):
        return jnp.where(b > col, col > 0, col < last)

    sums = []

    def sum_edge(phase, b, h):
        launch(sum_copy(phase, b, h), jnp.logical_not(fed(b)), sums)

    def sum_step(phase, b, h):
        copy = sum_copy(phase, b, h)

        @pl.when(fed(b))
        def _():
            side = jnp.where(b > col, 0, 1)
            copy.wait_recv()
            held = stage[b, rows_of(h)].astype(f32) + slots[side, b, rows_of(h)].astype(f32)
            stage[b, rows_of(h)] = held.astype(stage.dtype)

        launch(copy, fed(b), sums)

    def sum_own(phase, h):
        for side, condition in ((0, col > 0), (1, col < last)):

            @pl.when(condition)
            def _():
                slot = slots.at[side, col, rows_of(h)]
                remote(
                    slot, slot, rs_send.at[phase, col, h], rs_recv.at[phase, side, col, h], (row, onward(col))
                ).wait_recv()
                own_sum[rows_of(h)] += slots[side, col, rows_of(h)].astype(f32)

    def norm_rows(source, gain, target, index, h):
        step = min(size, 32)
        for start in range(h * size, (h + 1) * size, step):
            rows = pl.ds(start, step)
            target[index, rows] = layer_norm(source[rows], gain[...]).astype(target.dtype)

    def columns(width, tile, body):
        def step(j, carry):
            body(pl.ds(pl.multiple_of(j * tile, tile), tile))
            return carry

        lax.fori_loop(0, width // tile, step, 0, unroll=True)

    loads[0].wait()
    norm_rows(tokens, gain_one, image, col, 0)

    across_ids = jnp.broadcast_to(ids_in[...], (tok, tok)).astype(f32)
    named = across_ids.T
    earlier = lax.broadcasted_iota(jnp.int32, (tok, tok), 0) < lax.broadcasted_iota(
        jnp.int32, (tok, tok), 1
    )
    rank = jnp.sum(jnp.where(earlier & (named == across_ids), 1.0, 0.0), axis=0, keepdims=True)
    code = across_ids[0:8] * capacity + rank
    codes[col] = code.astype(jnp.int32)

    pl.semaphore_wait(barrier, row_total + col_total - 2)
    spread_start(0, 0)
    gather_start(0)
    gather_start(1)
    for h in range(1, parts):
        norm_rows(tokens, gain_one, image, col, h)
        spread_start(0, h)
    launch(code_copy(col, lax.rem(col + 1, col_total), 0), col < last)
    launch(code_copy(col, lax.rem(col + last, col_total), 1), col > 0)

    def project(b):
        def tile(at):
            inner = matmul(image[b], qkv[:, at])
            proj[pl.ds(pl.multiple_of(b * tok, tok), tok), at] = inner.astype(proj.dtype)

        columns(qkv.shape[1], 512, tile)

    def arrive(distance):
        for h in range(parts):
            spread_at(0, distance, h)
        for other in (col - distance, col + distance):
            valid = (other >= 0) & (other <= last)
            b = lax.rem(other + col_total, col_total)
            copy = code_copy(b, onward(b), 0)
            pl.when(valid)(copy.wait_recv)
            launch(copy, valid & more(b))

    for distance in range(1, max(2, last - 1)):
        arrive(distance)
    gather_relay(0)
    gather_relay(1)
    gather_start(2)
    for distance in range(max(2, last - 1), last):
        arrive(distance)
    gather_finish(0)
    gather_finish(1)
    gather_complete(0)
    gather_complete(1)
    for k in range(last):
        project(near[k])
    gather_relay(2)
    gather_start(3)
    gather_start(4)
    gather_start(5)
    if last > 1:
        arrive(last)
    project(near[last])
    gather_finish(2)

    def attend(b):
        mine = pl.ds(pl.multiple_of(b * tok, tok), tok)
        for n in range(heads):
            base, jump = n * head_dim, heads * head_dim
            query = proj[mine, base : base + head_dim]
            keys = proj[:, base + jump : base + jump + head_dim]
            values = proj[:, base + 2 * jump : base + 2 * jump + head_dim]
            scores = lax.dot_general(
                query, keys, (((1,), (1,)), ((), ())), preferred_element_type=f32
            )
            scores = scores * (head_dim ** (-0.5))
            weights = jnp.exp(scores - jnp.max(scores, axis=-1, keepdims=True))
            weights = weights / jnp.sum(weights, axis=-1, keepdims=True)
            attended[:, n * head_dim : (n + 1) * head_dim] = matmul(
                weights.astype(jnp.bfloat16), values
            ).astype(jnp.bfloat16)

    def head_terms(b, store):
        def tile(at):
            store(at, matmul(attended[...], outw[:, at]))

        columns(model, 512, tile)

    def to_stage(b):
        def store(at, inner):
            stage[b, :, at] = inner.astype(stage.dtype)

        return store

    def to_own(at, inner):
        own_sum[:, at] = inner

    for k in range(last):
        attend(far[k])
        if k == 0:
            gather_complete(2)
        head_terms(far[k], to_stage(far[k]))
        sum_edge(0, far[k], 0)
    for k in range(last):
        sum_edge(0, far[k], 1)

    def placing(b):
        slot = lax.broadcasted_iota(jnp.int32, (row_total * capacity, tok), 0)
        wanted = slot + lax.div(col, 2) * capacity
        for n in range(1, row_total):
            wanted += jnp.where(slot >= n * capacity, (col_total // 2 - 1) * capacity, 0)
        return jnp.where(wanted == codes[b][0:1], 1.0, 0.0)

    def group(index):
        return pl.ds(pl.multiple_of(index * capacity, capacity), capacity)

    def out_copy(b, source, target):
        return remote(
            table.at[b, group(target)],
            landed.at[b, group(source)],
            out_send.at[b, target],
            out_recv.at[b, source],
            (target, col),
        )

    def back_copy(b, holder, target):
        return remote(
            landed.at[b, group(target)],
            returned.at[b, group(holder)],
            back_send.at[b, target],
            back_recv.at[b, holder],
            (target, col),
        )

    def dispatch(b):
        place = placing(b).astype(jnp.bfloat16)

        def tile(at):
            table[b, :, at] = matmul(place, fresh[b, :, at]).astype(table.dtype)

        columns(model, 512, tile)
        for flip in (2, 4, 6, 3, 5, 7, 1):
            launch(out_copy(b, row, lax.bitwise_xor(row, flip)))
        landed[b, group(row)] = table[b, group(row)]

    def with_gelu(inner):
        return (inner * (1.0 + lax.erf(inner * (0.5**0.5))) * 0.5).astype(jnp.bfloat16)

    def expert(b):
        for flip in range(1, row_total):
            other = lax.bitwise_xor(row, flip)
            out_copy(b, other, row).wait_recv()

        def up(at):
            units[:, at] = with_gelu(matmul(landed[b], first[:, at]))

        columns(first.shape[1], 512, up)

        def down(at):
            landed[b, :, at] = matmul(units[...], second[:, at]).astype(landed.dtype)

        columns(model, 512, down)
        for flip in (2, 4, 6, 3, 5, 7, 1):
            launch(back_copy(b, row, lax.bitwise_xor(row, flip)))
        returned[b, group(row)] = landed[b, group(row)]

    def dense_up(b):
        def up(at):
            inner_units[:, at] = with_gelu(matmul(fresh[b], upw[:, at]))

        columns(upw.shape[1], 512, up)

    def dense_down(store):
        def down(at):
            store(at, matmul(inner_units[...], downw[:, at]))

        columns(model, 512, down)

    def dense(b, store):
        dense_up(b)
        dense_down(store)

    def combine(b, own):
        for flip in range(1, row_total):
            other = lax.bitwise_xor(row, flip)
            back_copy(b, other, row).wait_recv()
        pick = placing(b).T.astype(jnp.bfloat16)

        def tile(at):
            inner = matmul(pick, returned[b, :, at])
            if own:
                own_sum[:, at] += inner
            else:
                stage[b, :, at] = (stage[b, :, at].astype(f32) + inner).astype(stage.dtype)

        columns(model, 512, tile)

    def close_hidden(h):
        sum_own(0, h)
        rows = rows_of(h)
        hidden[rows] = (tokens[rows].astype(f32) + own_sum[rows]).astype(hidden.dtype)
        norm_rows(hidden, gain_two, fresh, col, h)
        spread_start(1, h)

    for k in range(last):
        sum_step(0, far[k], 0)
    attend(col)
    head_terms(col, to_own)
    def even_hops(h):
        for distance in range(2, last + 1, 2):
            if 0 <= h - distance // 2 - 1 < parts:
                spread_at(1, distance, h - distance // 2 - 1)

    def odd_hops(h, first_hop):
        for distance in range(1 if first_hop else 3, 2 if first_hop else last + 1, 2):
            if 0 <= h - (distance + 1) // 2 < parts:
                spread_at(1, distance, h - (distance + 1) // 2)

    def send_on(b):
        combine(b, False)
        for h in range(parts):
            sum_edge(1, b, h)

    for h in range(parts):
        if h > 0:
            for k in range(last):
                sum_step(0, far[k], h)
        even_hops(h)
        close_hidden(h)
        if h + 2 < parts:
            for k in range(last):
                sum_edge(0, far[k], h + 2)
        odd_hops(h, True)
        odd_hops(h, False)
        if h == parts // 4:
            gather_relay(3)
        if h == parts - 2:
            gather_relay(4)
    even_hops(parts)
    odd_hops(parts, True)
    dispatch(near[1])
    gather_relay(5)
    odd_hops(parts, False)
    gather_finish(3)
    even_hops(parts + 1)
    dispatch(near[2])
    odd_hops(parts + 1, False)
    drain(sums)
    loads[7].wait()
    loads[8].wait()
    gather_finish(4)
    expert(near[1])
    dispatch(near[3])
    gather_complete(3)
    dense_up(near[1])
    gather_finish(5)
    gather_complete(4)
    gather_complete(5)
    dense_down(to_stage(near[1]))
    expert(near[2])
    dispatch(col)
    send_on(near[1])
    dense(near[2], to_stage(near[2]))
    expert(near[3])
    send_on(near[2])
    dense(near[3], to_stage(near[3]))
    sum_step(1, late[0], 0)
    expert(col)
    for h in range(1, parts - 1):
        sum_step(1, late[0], h)
    send_on(near[3])
    sum_step(1, late[0], parts - 1)
    dense(col, to_own)
    sum_step(1, late[1], 0)
    combine(col, True)
    for h in range(1, parts + 1):
        if h < parts:
            sum_step(1, late[1], h)
        sum_step(1, late[2], h - 1)
    for h in range(parts):
        sum_own(1, h)
        rows = rows_of(h)
        result[rows] = (hidden[rows].astype(f32) + own_sum[rows]).astype(result.dtype)
    drain(sums)
    drain(finish)


def fused_block(tokens, gain_one, qkv_part, out_part, gain_two, up_part, down_part, ids, first, second, capacity, heads):
    row_total = lax.axis_size("row")
    col_total = lax.axis_size("col")
    tok, model = tokens.shape
    parts = 4
    hbm, vmem = pl.BlockSpec(memory_space=pl.ANY), pl.BlockSpec(memory_space=pltpu.VMEM)
    bf16 = jnp.bfloat16
    three = qkv_part.shape[1]
    width = out_part.shape[0]
    slot_count = row_total * capacity
    dma = pltpu.SemaphoreType.DMA
    scratch = [
        pltpu.VMEM((tok, model), bf16),
        pltpu.VMEM((col_total, tok, model), bf16),
        pltpu.VMEM((col_total, tok, model), bf16),
        pltpu.VMEM((row_total * qkv_part.shape[0], three), bf16),
        pltpu.VMEM((width, row_total * out_part.shape[1]), bf16),
        pltpu.VMEM((row_total * up_part.shape[0], up_part.shape[1]), bf16),
        pltpu.VMEM((down_part.shape[0], row_total * down_part.shape[1]), bf16),
        pltpu.VMEM(first.shape, bf16),
        pltpu.VMEM(second.shape, bf16),
        pltpu.VMEM((col_total * tok, three), bf16),
        pltpu.VMEM((tok, width), bf16),
        pltpu.VMEM((col_total, tok, model), bf16),
        pltpu.VMEM((2, col_total, tok, model), bf16),
        pltpu.VMEM((tok, model), jnp.float32),
        pltpu.VMEM((tok, model), bf16),
        pltpu.VMEM((col_total, slot_count, model), bf16),
        pltpu.VMEM((col_total, slot_count, model), bf16),
        pltpu.VMEM((col_total, slot_count, model), bf16),
        pltpu.VMEM((tok, first.shape[1]), bf16),
        pltpu.VMEM((tok, up_part.shape[1]), bf16),
        pltpu.VMEM((col_total, 8, tok), jnp.int32),
        dma((9,)),
        dma((2, col_total, parts, 2)),
        dma((2, col_total, parts)),
        dma((col_total, 2)),
        dma((col_total,)),
        dma((2, col_total, parts)),
        dma((2, 2, col_total, parts)),
        dma((6, 9)),
        dma((6, 9)),
        dma((col_total, row_total)),
        dma((col_total, row_total)),
        dma((col_total, row_total)),
        dma((col_total, row_total)),
    ]
    return pl.pallas_call(
        functools.partial(block_body, (row_total, col_total, capacity, heads, parts)),
        out_shape=jax.ShapeDtypeStruct((tok, model), bf16),
        in_specs=[hbm, vmem, vmem, vmem] + [hbm] * 6,
        out_specs=vmem,
        scratch_shapes=scratch,
        compiler_params=pltpu.CompilerParams(
            collective_id=0, has_side_effects=True, vmem_limit_bytes=62 * 2**20
        ),
        name="block",
    )(
        tokens,
        gain_one.reshape(1, model),
        gain_two.reshape(1, model),
        ids,
        qkv_part,
        out_part,
        up_part,
        down_part,
        first,
        second,
    )


def shards(
    tokens,
    ln1_gain,
    qkv_weight,
    out_weight,
    ln2_gain,
    ffn_in,
    ffn_out,
    expert_ids,
    expert_in,
    expert_out,
):
    tok_count, model_width = tokens.shape
    row_total = lax.axis_size("row")
    col_total = lax.axis_size("col")
    row_index = lax.axis_index("row")
    col_index = lax.axis_index("col")
    expert_count = row_total * col_total // 2
    capacity = max(2, 2 * tok_count // expert_count)
    head_count, head_dim = qkv_weight.shape[1], qkv_weight.shape[3]
    seq_len = tok_count * col_total
    if row_total == 8 and col_total == 4 and capacity % 16 == 0:
        return fused_block(
            tokens,
            ln1_gain,
            jnp.swapaxes(qkv_weight, 1, 2).reshape(qkv_weight.shape[0], -1),
            out_weight,
            ln2_gain,
            ffn_in,
            ffn_out,
            expert_ids.reshape(1, tok_count),
            expert_in[0],
            expert_out[0],
            capacity,
            head_count,
        )

    ids_block = jnp.broadcast_to(expert_ids[:, 0][None, :], (8, tok_count))
    qkv_whole, out_whole, image_rows, ids_all = exchange(
        "enter",
        0,
        gathers=((qkv_weight.reshape(qkv_weight.shape[0], -1), 0), (out_weight, 1)),
        spreads=(tokens, ids_block),
    )
    normed = layer_norm(image_rows, ln1_gain).astype(jnp.bfloat16)
    projected = matmul(normed, qkv_whole).astype(jnp.bfloat16)
    projected = projected.reshape(seq_len, head_count, 3, head_dim)
    queries, keys, values = projected[:, :, 0], projected[:, :, 1], projected[:, :, 2]
    scores = jnp.einsum("qhd,khd->hqk", queries, keys, preferred_element_type=jnp.float32)
    scores = scores * (head_dim ** (-0.5))
    weights = jnp.exp(scores - jnp.max(scores, axis=-1, keepdims=True))
    probabilities = (weights / jnp.sum(weights, axis=-1, keepdims=True)).astype(jnp.bfloat16)
    attended = jnp.einsum("hqk,khd->qhd", probabilities, values, preferred_element_type=jnp.float32)
    attended = attended.astype(jnp.bfloat16).reshape(seq_len, head_count * head_dim)
    head_terms = matmul(attended, out_whole).astype(jnp.bfloat16)
    head_terms = head_terms.reshape(col_total, tok_count, model_width)

    up_whole, mixed_heads = exchange("heads", 1, gathers=((ffn_in, 0),), sums=(head_terms,))
    hidden_mine = (tokens.astype(jnp.float32) + mixed_heads).astype(jnp.bfloat16)
    normed_mine = layer_norm(hidden_mine, ln2_gain).astype(jnp.bfloat16)

    down_whole, normed_image = exchange(
        "norms", 2, gathers=((ffn_out, 1),), spreads=(normed_mine,)
    )

    ids_rows = ids_all.reshape(col_total, 8, tok_count)[:, 0]
    expert_range = jnp.arange(expert_count, dtype=jnp.int32)
    one_hot = (ids_rows[:, :, None] == expert_range).astype(jnp.int32)
    earlier = jnp.cumsum(one_hot, axis=1) - one_hot
    slot_index = jnp.sum(earlier * one_hot, axis=2)
    block_index = jnp.arange(col_total, dtype=jnp.int32)[:, None]
    home_row = 2 * ids_rows // col_total
    mine = (2 * ids_rows % col_total) // 2 == col_index // 2
    step = (home_row - row_index + row_total) % row_total
    position = (step * col_total + block_index) * capacity + slot_index
    position = jnp.where(mine, position, -1).reshape(seq_len)
    slot_count = row_total * col_total * capacity
    slots = jnp.arange(slot_count, dtype=jnp.int32)
    placing = (slots[:, None] == position[None, :]).astype(jnp.bfloat16)
    picking = (position[:, None] == slots[None, :]).astype(jnp.bfloat16)

    table = matmul(placing, normed_image).astype(jnp.bfloat16)
    table = table.reshape(row_total, col_total * capacity, model_width)
    expert_rows, hidden_units = exchange(
        "dispatch", 3, shuffles=((table, 1),), units=((normed_image, up_whole, True),)
    )
    expert_units = up_gelu(expert_rows.reshape(slot_count, model_width), expert_in[0])
    partial_out = matmul(expert_units, expert_out[0]).astype(jnp.bfloat16)
    partial_out = partial_out.reshape(row_total, col_total * capacity, model_width)
    returned, dense_part = exchange(
        "collect", 4, shuffles=((partial_out, -1),), units=((hidden_units, down_whole, False),)
    )

    rows_two = returned.reshape(slot_count, model_width)
    partial = dense_part.astype(jnp.float32) + matmul(picking, rows_two)
    partial = partial.astype(jnp.bfloat16).reshape(col_total, tok_count, model_width)
    (total,) = exchange("leave", 5, sums=(partial,))
    return (hidden_mine.astype(jnp.float32) + total).astype(jnp.bfloat16)


def solution(mesh):
    in_specs = (
        P(("row", "col"), None),
        P(),
        P("row", "col", None, None),
        P("col", "row"),
        P(),
        P("row", "col"),
        P("col", "row"),
        P(("row", "col"), None),
        P(("row", "col"), None, None),
        P(("row", "col"), None, None),
    )
    out_specs = P(("row", "col"), None)
    return jax.shard_map(shards, mesh=mesh, in_specs=in_specs, out_specs=out_specs, check_vma=False)
```

```python
import functools
import jax
import jax.numpy as jnp
from jax import lax
from jax.experimental import pallas as pl
from jax.experimental.pallas import tpu as pltpu
from jax.sharding import PartitionSpec as P

MESH = pl.DeviceIdType.MESH


def flipped(index, bit):
    return index + bit - 2 * bit * ((index // bit) % 2)


def comm_body(plan, row_total, col_total, *refs):
    gathers, spreads, sums, shuffles, units = plan
    count = len(gathers) + len(spreads) + len(sums) + len(shuffles)
    ins, refs = refs[:count], refs[count:]
    operands, refs = refs[: 2 * len(units)], refs[2 * len(units) :]
    outs, refs = refs[:count], refs[count:]
    results, refs = refs[: len(units)], refs[len(units) :]
    stages, refs = refs[:count], refs[count:]
    sum_slots = refs[: 2 * len(sums)]
    send, recv, local = refs[2 * len(sums) :]
    row = lax.axis_index("row")
    col = lax.axis_index("col")

    barrier = pltpu.get_barrier_semaphore()
    peers = 0
    if gathers or shuffles:
        for step in range(1, row_total):
            pl.semaphore_signal(
                barrier, inc=1, device_id=(lax.rem(row + step, row_total), col), device_id_type=MESH
            )
            peers += 1
    if spreads or sums:
        for step in range(1, col_total):
            pl.semaphore_signal(
                barrier, inc=1, device_id=(row, lax.rem(col + step, col_total)), device_id_type=MESH
            )
            peers += 1

    loads = []
    for i in range(count):
        load = pltpu.make_async_copy(ins[i], stages[i], local.at[i])
        load.start()
        loads.append(load)
    pl.semaphore_wait(barrier, peers)

    serial = [0]
    finish = []
    pending = []
    kept = []

    def number():
        serial[0] += 1
        return serial[0] - 1

    def remote(k, src, dst, device):
        return pltpu.make_async_remote_copy(
            src, dst, send.at[k], recv.at[k], device_id=device, device_id_type=MESH
        )

    def copy(src, dst, arriving, device):
        k = number()
        out = remote(k, src, dst, device)
        out.start()
        finish.append((None, out))
        return remote(k, src, arriving, device)

    def copy_if(condition, k, src, dst, device):
        out = remote(k, src, dst, device)
        pl.when(condition)(out.start)
        finish.append((condition, out))

    def keep(i, src, dst):
        own = pltpu.make_async_copy(src, dst, local.at[count + i])
        own.start()
        kept.append(own)

    right = (row, lax.rem(col + 1, col_total))
    left = (row, lax.rem(col + col_total - 1, col_total))
    last = col_total - 1
    lines = []
    base = len(gathers)
    for i in range(base, base + len(spreads)):
        loads[i].wait()
        size = ins[i].shape[0]

        def block(index, i=i, size=size):
            index = lax.rem(index + col_total, col_total)
            return outs[i].at[pl.ds(pl.multiple_of(index * size, size), size)]

        keys = [(number(), number()) for _ in range(last)]
        copy_if(col < last, keys[0][0], stages[i], block(col), right)
        copy_if(col > 0, keys[0][1], stages[i], block(col), left)
        keep(i, stages[i], block(col))

        def advance(step, block=block, keys=keys):
            got = block(col - 1 - step)
            pl.when(col > step)(remote(keys[step][0], got, got, right).wait_recv)
            if step + 1 < last:
                copy_if((col > step) & (col < last), keys[step + 1][0], got, got, right)
            got = block(col + 1 + step)
            pl.when(col + step < last)(remote(keys[step][1], got, got, left).wait_recv)
            if step + 1 < last:
                copy_if((col + step < last) & (col > 0), keys[step + 1][1], got, got, left)

        lines.append(advance)
    base += len(spreads)
    for j in range(len(sums)):
        i = base + j
        loads[i].wait()
        stage, total = stages[i], outs[i]
        slots, merged = sum_slots[2 * j], sum_slots[2 * j + 1]
        keys = [number() for _ in range(col_total)]
        merge = col_total >= 4
        if merge:
            key = number()
            copy_if(col == 0, key, stage.at[last], merged, right)
            copy_if(col == last, key, stage.at[0], merged, left)

        def send_block(target, condition, source, stage=stage, slots=slots, keys=keys):
            out = pltpu.make_async_remote_copy(
                source,
                slots.at[col],
                send.at[keys[target]],
                recv.at[keys[0] + col],
                device_id=(row, target),
                device_id_type=MESH,
            )
            pl.when(condition)(out.start)
            finish.append((condition, out))

        for target in range(col_total):
            condition = col != target
            if merge and target == last:
                condition = condition & (col > 1)
            if merge and target == 0:
                condition = condition & (col < last - 1)
            send_block(target, condition, stage.at[target])
        total[...] = stage[pl.ds(col, 1)][0].astype(jnp.float32)

        def combine(stage=stage, merged=merged, key=key if merge else 0, send_block=send_block):
            for target, holder in ((last, 1), (0, last - 1)):
                pl.when(col == holder)(remote(key, merged, merged, right).wait_recv)

                @pl.when(col == holder)
                def _():
                    merged[...] = (
                        merged[...].astype(jnp.float32) + stage[target].astype(jnp.float32)
                    ).astype(merged.dtype)

                send_block(target, col == holder, merged)

        def collect(total=total, slots=slots, keys=keys, merge=merge):
            for source in range(col_total):
                condition = col != source
                if merge and source == 0:
                    condition = condition & (col < last)
                if merge and source == last:
                    condition = condition & (col > 0)
                slot = slots.at[source]
                pl.when(condition)(remote(keys[source], slot, slot, right).wait_recv)

                @pl.when(condition)
                def _():
                    total[...] += slots[source].astype(jnp.float32)

        def advance(step, combine=combine, collect=collect, merge=merge):
            if step == 0 and merge:
                combine()
            if step == last - 1:
                collect()

        lines.append(advance)
    base += len(sums)
    for i in range(base, base + len(shuffles)):
        loads[i].wait()
        for step in range(1, row_total):
            to = lax.rem(row + (step if shuffles[i - base] > 0 else row_total - step), row_total)
            slot = outs[i].at[step]
            pending.append(copy(stages[i].at[step], slot, slot, (to, col)))
        keep(i, stages[i].at[0], outs[i].at[0])

    partner = flipped(row, 1)
    relay = row_total == 8

    def piece(i, index, half):
        depth, width = ins[i].shape
        start, size = (0, depth) if half is None else (half * (depth // 2), depth // 2)
        if gathers[i] == 0:
            return outs[i].at[pl.ds(pl.multiple_of(index * depth + start, size), size)]
        return outs[i].at[pl.ds(start, size), pl.ds(pl.multiple_of(index * width, width), width)]

    arrivals = []
    for i in range(len(gathers)):
        loads[i].wait()
        mine = piece(i, row, None)
        if relay:
            sources = [flipped(row, 2), flipped(row, 4)]
            targets = sources
        else:
            sources = [lax.rem(row + row_total - 2 * d, row_total) for d in range(1, row_total // 2)]
            targets = [lax.rem(row + 2 * d, row_total) for d in range(1, row_total // 2)]
        first = [
            (source, copy(stages[i], mine, piece(i, source, None), (target, col)))
            for source, target in zip(sources, targets)
        ]
        pending.append(copy(stages[i], mine, piece(i, partner, None), (partner, col)))
        keep(i, stages[i], mine)
        arrivals.append(first)

    def hand_on(i, source, half):
        got = piece(i, source, half)
        pending.append(copy(got, got, piece(i, flipped(source, 1), half), (partner, col)))

    seconds = []

    def first_level(i):
        if not relay:
            for source, arrival in arrivals[i]:
                arrival.wait_recv()
                hand_on(i, source, None)
            return
        (by_x, from_x), (by_y, from_y) = arrivals[i]
        across = flipped(by_x, 4)
        from_x.wait_recv()
        got = piece(i, by_x, 0)
        diag_a = copy(got, got, piece(i, across, 0), (by_y, col))
        hand_on(i, by_x, None)
        from_y.wait_recv()
        got = piece(i, by_y, 1)
        diag_b = copy(got, got, piece(i, across, 1), (by_x, col))
        hand_on(i, by_y, None)
        seconds.append((i, across, diag_a, diag_b))

    early = len(gathers) // 2 if lines else 0
    for step in range(last if lines else 0):
        for advance in lines:
            advance(step)
        if step == 0:
            for i in range(early):
                first_level(i)
        if step == min(1, last - 1):
            for i in range(early, len(gathers)):
                first_level(i)
    if not lines:
        for i in range(len(gathers)):
            first_level(i)
    for n in range(len(units)):
        x_ref, w_ref, o_ref = operands[2 * n], operands[2 * n + 1], results[n]
        rows, depth = x_ref.shape
        width = w_ref.shape[1]
        tile = min(width, 256)
        pltpu.emit_pipeline(
            up_body if units[n] else plain_body,
            grid=(width // tile,),
            in_specs=[
                pl.BlockSpec((rows, depth), lambda j: (0, 0)),
                pl.BlockSpec((depth, tile), lambda j: (0, j)),
            ],
            out_specs=[pl.BlockSpec((rows, tile), lambda j: (0, j))],
        )(x_ref, w_ref, o_ref)
    for i, across, diag_a, diag_b in seconds:
        for half, arrival in ((0, diag_a), (1, diag_b)):
            arrival.wait_recv()
            hand_on(i, across, half)
    for arrival in pending:
        arrival.wait_recv()
    for condition, out in finish:
        if condition is None:
            out.wait_send()
        else:
            pl.when(condition)(out.wait_send)
    for own in kept:
        own.wait()


def exchange(name, collective_id, gathers=(), spreads=(), sums=(), shuffles=(), units=()):
    row_total = lax.axis_size("row")
    col_total = lax.axis_size("col")
    arrays, shapes, copies = [], [], 0
    hbm, vmem = pl.BlockSpec(memory_space=pl.ANY), pl.BlockSpec(memory_space=pltpu.VMEM)
    for array, axis in gathers:
        depth, width = array.shape
        arrays.append(array)
        shape = (depth * row_total, width) if axis == 0 else (depth, width * row_total)
        shapes.append((shape, array.dtype, hbm))
        copies += 9 if row_total == 8 else row_total
    for array in spreads:
        arrays.append(array)
        shape = (array.shape[0] * col_total,) + array.shape[1:]
        shapes.append((shape, array.dtype, hbm))
        copies += 2 * (col_total - 1)
    slots = []
    for array in sums:
        arrays.append(array)
        shapes.append((array.shape[1:], jnp.float32, vmem))
        slots += [pltpu.VMEM(array.shape, array.dtype), pltpu.VMEM(array.shape[1:], array.dtype)]
        copies += col_total + 1
    for array, _ in shuffles:
        arrays.append(array)
        shapes.append((array.shape, array.dtype, hbm))
        copies += row_total - 1
    operands = []
    for x, w, _ in units:
        operands += [x, w]
        shapes.append(((x.shape[0], w.shape[1]), jnp.bfloat16, hbm))
    plan = (
        [axis for _, axis in gathers],
        [0] * len(spreads),
        [0] * len(sums),
        [sign for _, sign in shuffles],
        [with_gelu for _, _, with_gelu in units],
    )
    return pl.pallas_call(
        functools.partial(comm_body, plan, row_total, col_total),
        out_shape=[jax.ShapeDtypeStruct(shape, dtype) for shape, dtype, _ in shapes],
        in_specs=[hbm] * (len(arrays) + len(operands)),
        out_specs=[spec for _, _, spec in shapes],
        scratch_shapes=[pltpu.VMEM(a.shape, a.dtype) for a in arrays]
        + slots
        + [
            pltpu.SemaphoreType.DMA((copies,)),
            pltpu.SemaphoreType.DMA((copies,)),
            pltpu.SemaphoreType.DMA((2 * len(arrays),)),
        ],
        compiler_params=pltpu.CompilerParams(
            collective_id=collective_id, has_side_effects=True, vmem_limit_bytes=16 * 2**20
        ),
        name=name,
    )(*arrays, *operands)


def plain_body(x_ref, w_ref, o_ref):
    inner = jnp.dot(x_ref[...], w_ref[...], preferred_element_type=jnp.float32)
    o_ref[...] = inner.astype(o_ref.dtype)


def up_body(x_ref, w_ref, o_ref):
    inner = jnp.dot(x_ref[...], w_ref[...], preferred_element_type=jnp.float32)
    o_ref[...] = (inner * (1.0 + lax.erf(inner * (0.5**0.5))) * 0.5).astype(o_ref.dtype)


def up_gelu(x, w):
    rows, depth = x.shape
    width = w.shape[1]
    tile = min(width, 256)
    return pl.pallas_call(
        up_body,
        grid=(width // tile,),
        out_shape=jax.ShapeDtypeStruct((rows, width), jnp.bfloat16),
        in_specs=[
            pl.BlockSpec((rows, depth), lambda j: (0, 0)),
            pl.BlockSpec((depth, tile), lambda j: (0, j)),
        ],
        out_specs=pl.BlockSpec((rows, tile), lambda j: (0, j)),
        compiler_params=pltpu.CompilerParams(vmem_limit_bytes=32 * 2**20),
        cost_estimate=pl.CostEstimate(
            flops=2 * rows * depth * width,
            bytes_accessed=2 * (rows * depth + depth * width + rows * width),
            transcendentals=0,
        ),
        name="up_gelu",
    )(x, w)


def layer_norm(row_data, gain_vector):
    row_data = row_data.astype(jnp.float32)
    centered = row_data - jnp.mean(row_data, axis=-1, keepdims=True)
    spread = jnp.mean(centered * centered, axis=-1, keepdims=True)
    return centered * lax.rsqrt(spread + 1e-06) * gain_vector


def matmul(a, b):
    return jnp.dot(a, b, preferred_element_type=jnp.float32)


def chosen(table, index):
    value = jnp.int32(table[0])
    for n in range(1, len(table)):
        value = jnp.where(index == n, jnp.int32(table[n]), value)
    return value


def near_first(total):
    return [sorted(range(total), key=lambda b: (abs(b - c), b)) for c in range(total)]


def far_first(total):
    last = total - 1
    return [
        sorted(range(total), key=lambda b: (-abs(b - c), c if b > c else last - c))
        for c in range(total)
    ]


def block_body(sizes, *refs):
    row_total, col_total, capacity, heads, parts = sizes
    (tokens_in, gain_one_in, gain_two_in, ids_in, qkv_in, out_in, up_in, down_in, first_in, second_in) = refs[:10]
    result_out = refs[10]
    (tokens, image, fresh, qkv, outw, upw, downw, first, second, proj, attended, stage, slots) = refs[11:24]
    (own_sum, hidden, table, landed, returned, units, inner_units, codes) = refs[24:32]
    (load_sem, ag_send, ag_recv, code_send, code_recv, rs_send, rs_recv) = refs[32:39]
    (gather_send, gather_recv, out_send, out_recv, back_send, back_recv) = refs[39:45]
    (gain_one, gain_two, ids, result, store_sem) = refs[45:]
    row = lax.axis_index("row")
    col = lax.axis_index("col")
    last = col_total - 1
    tok, model = tokens.shape
    size = tok // parts
    head_dim = attended.shape[1] // heads
    f32 = jnp.float32

    barrier = pltpu.get_barrier_semaphore()
    for step in range(1, row_total):
        pl.semaphore_signal(
            barrier, inc=1, device_id=(lax.rem(row + step, row_total), col), device_id_type=MESH
        )
    for step in range(1, col_total):
        pl.semaphore_signal(
            barrier, inc=1, device_id=(row, lax.rem(col + step, col_total)), device_id_type=MESH
        )

    finish = []

    def remote(src, dst, send, recv, device):
        return pltpu.make_async_remote_copy(
            src, dst, send, recv, device_id=device, device_id_type=MESH
        )

    def launch(copy, condition=None, into=None):
        if condition is None:
            copy.start()
        else:
            pl.when(condition)(copy.start)
        (finish if into is None else into).append((condition, copy))

    def drain(items):
        for condition, copy in items:
            if condition is None:
                copy.wait_send()
            else:
                pl.when(condition)(copy.wait_send)
        items.clear()

    cut = qkv_in.shape[0] // 2
    wholes = [
        (qkv, qkv_in, 0, 0, cut),
        (qkv, qkv_in, 0, cut, cut),
        (outw, out_in, 1, 0, out_in.shape[0]),
        (upw, up_in, 0, 0, up_in.shape[0]),
        (downw, down_in, 1, 0, down_in.shape[0] // 2),
        (downw, down_in, 1, down_in.shape[0] // 2, down_in.shape[0] // 2),
    ]

    def piece(g, index, half=None):
        whole, part, axis, start, count = wholes[g]
        depth, width = part.shape
        if half is not None:
            start, count = start + half * (count // 2), count // 2
        if axis == 0:
            return whole.at[pl.ds(pl.multiple_of(index * depth + start, count), count)]
        return whole.at[pl.ds(start, count), pl.ds(pl.multiple_of(index * width, width), width)]

    loads = [pltpu.make_async_copy(tokens_in, tokens, load_sem.at[0])]
    for g, (_, part, _, start, count) in enumerate(wholes):
        source = part.at[pl.ds(start, count)]
        loads.append(pltpu.make_async_copy(source, piece(g, row), load_sem.at[1 + g]))
    loads.append(pltpu.make_async_copy(first_in, first, load_sem.at[7]))
    loads.append(pltpu.make_async_copy(second_in, second, load_sem.at[8]))
    small = [
        pltpu.make_async_copy(gain_one_in, gain_one, load_sem.at[9]),
        pltpu.make_async_copy(ids_in, ids, load_sem.at[10]),
        pltpu.make_async_copy(gain_two_in, gain_two, load_sem.at[11]),
    ]
    for load in loads[:1] + small + loads[1:]:
        load.start()

    partner, by_x, by_y = flipped(row, 1), flipped(row, 2), flipped(row, 4)
    across = flipped(by_x, 4)

    def gather_copy(g, key, index, half, target):
        part = piece(g, index, half)
        return remote(part, part, gather_send.at[g, key], gather_recv.at[g, key], (target, col))

    def gather_wait(g, key, index, half=None):
        gather_copy(g, key, index, half, partner).wait_recv()

    def gather_start(g):
        loads[1 + g].wait()
        launch(gather_copy(g, 0, row, None, by_x))
        launch(gather_copy(g, 1, row, None, by_y))
        launch(gather_copy(g, 2, row, None, partner))

    def gather_relay(g):
        gather_wait(g, 0, by_x)
        launch(gather_copy(g, 3, by_x, 0, by_y))
        launch(gather_copy(g, 5, by_x, None, partner))
        gather_wait(g, 1, by_y)
        launch(gather_copy(g, 4, by_y, 1, by_x))
        launch(gather_copy(g, 6, by_y, None, partner))

    def gather_finish(g):
        gather_wait(g, 3, across, 0)
        launch(gather_copy(g, 7, across, 0, partner))
        gather_wait(g, 4, across, 1)
        launch(gather_copy(g, 8, across, 1, partner))

    def gather_complete(g):
        gather_wait(g, 2, partner)
        gather_wait(g, 5, flipped(by_x, 1))
        gather_wait(g, 6, flipped(by_y, 1))
        gather_wait(g, 7, flipped(across, 1), 0)
        gather_wait(g, 8, flipped(across, 1), 1)

    near = [chosen([order[k] for order in near_first(col_total)], col) for k in range(col_total)]
    far = [chosen([order[k] for order in far_first(col_total)], col) for k in range(col_total)]

    def rows_of(h):
        return pl.ds(h * size, size)

    def spread_copy(phase, b, h, target, way):
        part = (image, fresh)[phase].at[b, rows_of(h)]
        return remote(
            part, part, ag_send.at[phase, b, h, way], ag_recv.at[phase, b, h], (row, target)
        )

    def spread_start(phase, h):
        launch(spread_copy(phase, col, h, lax.rem(col + 1, col_total), 0), col < last)
        launch(spread_copy(phase, col, h, lax.rem(col + last, col_total), 1), col > 0)

    def onward(b):
        return jnp.where(b < col, lax.rem(col + 1, col_total), lax.rem(col + last, col_total))

    def more(b):
        return jnp.where(b < col, col < last, col > 0)

    def spread_at(phase, distance, h):
        for other in (col - distance, col + distance):
            valid = (other >= 0) & (other <= last)
            b = lax.rem(other + col_total, col_total)
            copy = spread_copy(phase, b, h, onward(b), 0)
            pl.when(valid)(copy.wait_recv)
            launch(copy, valid & more(b))

    def code_copy(b, target, way):
        return remote(
            codes.at[b], codes.at[b], code_send.at[b, way], code_recv.at[b], (row, target)
        )

    def sum_copy(phase, b, h):
        side = jnp.where(b > col, 0, 1)
        target = jnp.where(b > col, lax.rem(col + 1, col_total), lax.rem(col + last, col_total))
        return remote(
            stage.at[b, rows_of(h)],
            slots.at[side, b, rows_of(h)],
            rs_send.at[phase, b, h],
            rs_recv.at[phase, side, b, h],
            (row, target),
        )

    def fed(b):
        return jnp.where(b > col, col > 0, col < last)

    sums = []

    def sum_edge(phase, b, h):
        launch(sum_copy(phase, b, h), jnp.logical_not(fed(b)), sums)

    def sum_step(phase, b, h):
        copy = sum_copy(phase, b, h)

        @pl.when(fed(b))
        def _():
            side = jnp.where(b > col, 0, 1)
            copy.wait_recv()
            held = stage[b, rows_of(h)].astype(f32) + slots[side, b, rows_of(h)].astype(f32)
            stage[b, rows_of(h)] = held.astype(stage.dtype)

        launch(copy, fed(b), sums)

    def sum_own(phase, h):
        for side, condition in ((0, col > 0), (1, col < last)):

            @pl.when(condition)
            def _():
                slot = slots.at[side, col, rows_of(h)]
                remote(
                    slot, slot, rs_send.at[phase, col, h], rs_recv.at[phase, side, col, h], (row, onward(col))
                ).wait_recv()
                own_sum[rows_of(h)] += slots[side, col, rows_of(h)].astype(f32)

    def norm_rows(source, gain, target, index, h):
        step = min(size, 32)
        for start in range(h * size, (h + 1) * size, step):
            rows = pl.ds(start, step)
            target[index, rows] = layer_norm(source[rows], gain[...]).astype(target.dtype)

    def columns(width, tile, body):
        def step(j, carry):
            body(pl.ds(pl.multiple_of(j * tile, tile), tile))
            return carry

        lax.fori_loop(0, width // tile, step, 0, unroll=True)

    loads[0].wait()
    for load in small:
        load.wait()
    norm_rows(tokens, gain_one, image, col, 0)

    across_ids = jnp.broadcast_to(ids[...], (tok, tok)).astype(f32)
    named = across_ids.T
    earlier = lax.broadcasted_iota(jnp.int32, (tok, tok), 0) < lax.broadcasted_iota(
        jnp.int32, (tok, tok), 1
    )
    rank = jnp.sum(jnp.where(earlier & (named == across_ids), 1.0, 0.0), axis=0, keepdims=True)
    code = across_ids[0:8] * capacity + rank
    codes[col] = code.astype(jnp.int32)

    pl.semaphore_wait(barrier, row_total + col_total - 2)
    spread_start(0, 0)
    gather_start(0)
    gather_start(1)
    for h in range(1, parts):
        norm_rows(tokens, gain_one, image, col, h)
        spread_start(0, h)
    launch(code_copy(col, lax.rem(col + 1, col_total), 0), col < last)
    launch(code_copy(col, lax.rem(col + last, col_total), 1), col > 0)

    def project(b):
        def tile(at):
            inner = matmul(image[b], qkv[:, at])
            proj[pl.ds(pl.multiple_of(b * tok, tok), tok), at] = inner.astype(proj.dtype)

        columns(qkv.shape[1], 512, tile)

    def arrive(distance):
        for h in range(parts):
            spread_at(0, distance, h)
        for other in (col - distance, col + distance):
            valid = (other >= 0) & (other <= last)
            b = lax.rem(other + col_total, col_total)
            copy = code_copy(b, onward(b), 0)
            pl.when(valid)(copy.wait_recv)
            launch(copy, valid & more(b))

    for distance in range(1, max(2, last - 1)):
        arrive(distance)
    gather_relay(0)
    gather_relay(1)
    gather_start(2)
    for distance in range(max(2, last - 1), last):
        arrive(distance)
    gather_finish(0)
    gather_finish(1)
    gather_complete(0)
    gather_complete(1)
    for k in range(last):
        project(near[k])
    gather_relay(2)
    gather_start(3)
    gather_start(4)
    gather_start(5)
    if last > 1:
        arrive(last)
    project(near[last])
    gather_finish(2)

    def attend(b):
        mine = pl.ds(pl.multiple_of(b * tok, tok), tok)
        for n in range(heads):
            base, jump = n * head_dim, heads * head_dim
            query = proj[mine, base : base + head_dim]
            keys = proj[:, base + jump : base + jump + head_dim]
            values = proj[:, base + 2 * jump : base + 2 * jump + head_dim]
            scores = lax.dot_general(
                query, keys, (((1,), (1,)), ((), ())), preferred_element_type=f32
            )
            scores = scores * (head_dim ** (-0.5))
            weights = jnp.exp(scores - jnp.max(scores, axis=-1, keepdims=True))
            weights = weights / jnp.sum(weights, axis=-1, keepdims=True)
            attended[:, n * head_dim : (n + 1) * head_dim] = matmul(
                weights.astype(jnp.bfloat16), values
            ).astype(jnp.bfloat16)

    def head_terms(b, store):
        def tile(at):
            store(at, matmul(attended[...], outw[:, at]))

        columns(model, 512, tile)

    def to_stage(b):
        def store(at, inner):
            stage[b, :, at] = inner.astype(stage.dtype)

        return store

    def to_own(at, inner):
        own_sum[:, at] = inner

    for k in range(last):
        attend(far[k])
        if k == 0:
            gather_complete(2)
        head_terms(far[k], to_stage(far[k]))
        sum_edge(0, far[k], 0)
    for k in range(last):
        sum_edge(0, far[k], 1)

    def placing(b):
        slot = lax.broadcasted_iota(jnp.int32, (row_total * capacity, tok), 0)
        wanted = slot + lax.div(col, 2) * capacity
        for n in range(1, row_total):
            wanted += jnp.where(slot >= n * capacity, (col_total // 2 - 1) * capacity, 0)
        return jnp.where(wanted == codes[b][0:1], 1.0, 0.0)

    def group(index):
        return pl.ds(pl.multiple_of(index * capacity, capacity), capacity)

    def out_copy(b, source, target):
        return remote(
            table.at[b, group(target)],
            landed.at[b, group(source)],
            out_send.at[b, target],
            out_recv.at[b, source],
            (target, col),
        )

    def back_copy(b, holder, target):
        return remote(
            landed.at[b, group(target)],
            returned.at[b, group(holder)],
            back_send.at[b, target],
            back_recv.at[b, holder],
            (target, col),
        )

    def dispatch(b):
        place = placing(b).astype(jnp.bfloat16)

        def tile(at):
            table[b, :, at] = matmul(place, fresh[b, :, at]).astype(table.dtype)

        columns(model, 512, tile)
        for flip in (2, 4, 6, 3, 5, 7, 1):
            launch(out_copy(b, row, lax.bitwise_xor(row, flip)))
        landed[b, group(row)] = table[b, group(row)]

    def with_gelu(inner):
        return (inner * (1.0 + lax.erf(inner * (0.5**0.5))) * 0.5).astype(jnp.bfloat16)

    def expert(b):
        for flip in range(1, row_total):
            other = lax.bitwise_xor(row, flip)
            out_copy(b, other, row).wait_recv()

        def up(at):
            units[:, at] = with_gelu(matmul(landed[b], first[:, at]))

        columns(first.shape[1], 512, up)

        def down(at):
            landed[b, :, at] = matmul(units[...], second[:, at]).astype(landed.dtype)

        columns(model, 512, down)
        for flip in (2, 4, 6, 3, 5, 7, 1):
            launch(back_copy(b, row, lax.bitwise_xor(row, flip)))
        returned[b, group(row)] = landed[b, group(row)]

    def dense_up(b):
        def up(at):
            inner_units[:, at] = with_gelu(matmul(fresh[b], upw[:, at]))

        columns(upw.shape[1], 512, up)

    def dense_down(store):
        def down(at):
            store(at, matmul(inner_units[...], downw[:, at]))

        columns(model, 512, down)

    def dense(b, store):
        dense_up(b)
        dense_down(store)

    def combine(b, own):
        for flip in range(1, row_total):
            other = lax.bitwise_xor(row, flip)
            back_copy(b, other, row).wait_recv()
        pick = placing(b).T.astype(jnp.bfloat16)

        def tile(at):
            inner = matmul(pick, returned[b, :, at])
            if own:
                own_sum[:, at] += inner
            else:
                stage[b, :, at] = (stage[b, :, at].astype(f32) + inner).astype(stage.dtype)

        columns(model, 512, tile)

    def close_hidden(h):
        sum_own(0, h)
        rows = rows_of(h)
        hidden[rows] = (tokens[rows].astype(f32) + own_sum[rows]).astype(hidden.dtype)
        norm_rows(hidden, gain_two, fresh, col, h)
        spread_start(1, h)

    for k in range(last):
        sum_step(0, far[k], 0)
    attend(col)
    head_terms(col, to_own)
    def even_hops(h):
        for distance in range(2, last + 1, 2):
            if 0 <= h - distance // 2 - 1 < parts:
                spread_at(1, distance, h - distance // 2 - 1)

    def odd_hops(h, first_hop):
        for distance in range(1 if first_hop else 3, 2 if first_hop else last + 1, 2):
            if 0 <= h - (distance + 1) // 2 < parts:
                spread_at(1, distance, h - (distance + 1) // 2)

    def send_on(b):
        combine(b, False)
        for h in range(parts):
            sum_edge(1, b, h)

    for h in range(parts):
        if h > 0:
            for k in range(last):
                sum_step(0, far[k], h)
        even_hops(h)
        close_hidden(h)
        if h + 2 < parts:
            for k in range(last):
                sum_edge(0, far[k], h + 2)
        odd_hops(h, True)
        odd_hops(h, False)
        if h == parts // 4:
            gather_relay(3)
        if h == parts - 2:
            gather_relay(4)
        if h == parts - 1:
            gather_relay(5)
    even_hops(parts)
    odd_hops(parts, True)
    odd_hops(parts, False)
    gather_finish(3)
    even_hops(parts + 1)
    odd_hops(parts + 1, False)
    dispatch(far[0])
    dispatch(far[1])
    drain(sums)
    gather_finish(4)
    gather_complete(3)
    dense_up(far[0])
    gather_finish(5)
    gather_complete(4)
    gather_complete(5)
    dense_down(to_stage(far[0]))
    dense(far[1], to_stage(far[1]))
    loads[7].wait()
    loads[8].wait()
    expert(far[0])
    dispatch(far[2])
    expert(far[1])
    dispatch(col)
    send_on(far[0])
    dense(far[2], to_stage(far[2]))
    dense(col, to_own)
    sum_step(1, far[0], 0)
    expert(far[2])
    for h in range(1, parts - 1):
        sum_step(1, far[0], h)
    send_on(far[1])
    sum_step(1, far[0], parts - 1)
    expert(col)
    for h in range(parts // 2):
        sum_step(1, far[1], h)
    send_on(far[2])
    for h in range(parts):
        sum_step(1, far[2], h)
    for h in range(parts // 2, parts):
        sum_step(1, far[1], h)
    combine(col, True)
    for h in range(parts):
        sum_own(1, h)
        rows = rows_of(h)
        result[rows] = (hidden[rows].astype(f32) + own_sum[rows]).astype(result.dtype)
        pltpu.make_async_copy(result.at[rows], result_out.at[rows], store_sem.at[h]).start()
    drain(sums)
    drain(finish)
    for h in range(parts):
        rows = rows_of(h)
        pltpu.make_async_copy(result.at[rows], result_out.at[rows], store_sem.at[h]).wait()


def fused_block(tokens, gain_one, qkv_part, out_part, gain_two, up_part, down_part, ids, first, second, capacity, heads):
    row_total = lax.axis_size("row")
    col_total = lax.axis_size("col")
    tok, model = tokens.shape
    parts = 4
    hbm = pl.BlockSpec(memory_space=pl.ANY)
    bf16 = jnp.bfloat16
    three = qkv_part.shape[1]
    width = out_part.shape[0]
    slot_count = row_total * capacity
    dma = pltpu.SemaphoreType.DMA
    scratch = [
        pltpu.VMEM((tok, model), bf16),
        pltpu.VMEM((col_total, tok, model), bf16),
        pltpu.VMEM((col_total, tok, model), bf16),
        pltpu.VMEM((row_total * qkv_part.shape[0], three), bf16),
        pltpu.VMEM((width, row_total * out_part.shape[1]), bf16),
        pltpu.VMEM((row_total * up_part.shape[0], up_part.shape[1]), bf16),
        pltpu.VMEM((down_part.shape[0], row_total * down_part.shape[1]), bf16),
        pltpu.VMEM(first.shape, bf16),
        pltpu.VMEM(second.shape, bf16),
        pltpu.VMEM((col_total * tok, three), bf16),
        pltpu.VMEM((tok, width), bf16),
        pltpu.VMEM((col_total, tok, model), bf16),
        pltpu.VMEM((2, col_total, tok, model), bf16),
        pltpu.VMEM((tok, model), jnp.float32),
        pltpu.VMEM((tok, model), bf16),
        pltpu.VMEM((col_total, slot_count, model), bf16),
        pltpu.VMEM((col_total, slot_count, model), bf16),
        pltpu.VMEM((col_total, slot_count, model), bf16),
        pltpu.VMEM((tok, first.shape[1]), bf16),
        pltpu.VMEM((tok, up_part.shape[1]), bf16),
        pltpu.VMEM((col_total, 8, tok), jnp.int32),
        dma((12,)),
        dma((2, col_total, parts, 2)),
        dma((2, col_total, parts)),
        dma((col_total, 2)),
        dma((col_total,)),
        dma((2, col_total, parts)),
        dma((2, 2, col_total, parts)),
        dma((6, 9)),
        dma((6, 9)),
        dma((col_total, row_total)),
        dma((col_total, row_total)),
        dma((col_total, row_total)),
        dma((col_total, row_total)),
        pltpu.VMEM((1, model), jnp.float32),
        pltpu.VMEM((1, model), jnp.float32),
        pltpu.VMEM((1, tok), jnp.int32),
        pltpu.VMEM((tok, model), bf16),
        dma((parts,)),
    ]
    return pl.pallas_call(
        functools.partial(block_body, (row_total, col_total, capacity, heads, parts)),
        out_shape=jax.ShapeDtypeStruct((tok, model), bf16),
        in_specs=[hbm] * 10,
        out_specs=hbm,
        scratch_shapes=scratch,
        compiler_params=pltpu.CompilerParams(
            collective_id=0, has_side_effects=True, vmem_limit_bytes=67043328
        ),
        name="block",
    )(
        tokens,
        gain_one.reshape(1, model),
        gain_two.reshape(1, model),
        ids,
        qkv_part,
        out_part,
        up_part,
        down_part,
        first,
        second,
    )


def shards(
    tokens,
    ln1_gain,
    qkv_weight,
    out_weight,
    ln2_gain,
    ffn_in,
    ffn_out,
    expert_ids,
    expert_in,
    expert_out,
):
    tok_count, model_width = tokens.shape
    row_total = lax.axis_size("row")
    col_total = lax.axis_size("col")
    row_index = lax.axis_index("row")
    col_index = lax.axis_index("col")
    expert_count = row_total * col_total // 2
    capacity = max(2, 2 * tok_count // expert_count)
    head_count, head_dim = qkv_weight.shape[1], qkv_weight.shape[3]
    seq_len = tok_count * col_total
    if row_total == 8 and col_total == 4 and capacity % 16 == 0:
        return fused_block(
            tokens,
            ln1_gain,
            jnp.swapaxes(qkv_weight, 1, 2).reshape(qkv_weight.shape[0], -1),
            out_weight,
            ln2_gain,
            ffn_in,
            ffn_out,
            expert_ids.reshape(1, tok_count),
            expert_in[0],
            expert_out[0],
            capacity,
            head_count,
        )

    ids_block = jnp.broadcast_to(expert_ids[:, 0][None, :], (8, tok_count))
    qkv_whole, out_whole, image_rows, ids_all = exchange(
        "enter",
        0,
        gathers=((qkv_weight.reshape(qkv_weight.shape[0], -1), 0), (out_weight, 1)),
        spreads=(tokens, ids_block),
    )
    normed = layer_norm(image_rows, ln1_gain).astype(jnp.bfloat16)
    projected = matmul(normed, qkv_whole).astype(jnp.bfloat16)
    projected = projected.reshape(seq_len, head_count, 3, head_dim)
    queries, keys, values = projected[:, :, 0], projected[:, :, 1], projected[:, :, 2]
    scores = jnp.einsum("qhd,khd->hqk", queries, keys, preferred_element_type=jnp.float32)
    scores = scores * (head_dim ** (-0.5))
    weights = jnp.exp(scores - jnp.max(scores, axis=-1, keepdims=True))
    probabilities = (weights / jnp.sum(weights, axis=-1, keepdims=True)).astype(jnp.bfloat16)
    attended = jnp.einsum("hqk,khd->qhd", probabilities, values, preferred_element_type=jnp.float32)
    attended = attended.astype(jnp.bfloat16).reshape(seq_len, head_count * head_dim)
    head_terms = matmul(attended, out_whole).astype(jnp.bfloat16)
    head_terms = head_terms.reshape(col_total, tok_count, model_width)

    up_whole, mixed_heads = exchange("heads", 1, gathers=((ffn_in, 0),), sums=(head_terms,))
    hidden_mine = (tokens.astype(jnp.float32) + mixed_heads).astype(jnp.bfloat16)
    normed_mine = layer_norm(hidden_mine, ln2_gain).astype(jnp.bfloat16)

    down_whole, normed_image = exchange(
        "norms", 2, gathers=((ffn_out, 1),), spreads=(normed_mine,)
    )

    ids_rows = ids_all.reshape(col_total, 8, tok_count)[:, 0]
    expert_range = jnp.arange(expert_count, dtype=jnp.int32)
    one_hot = (ids_rows[:, :, None] == expert_range).astype(jnp.int32)
    earlier = jnp.cumsum(one_hot, axis=1) - one_hot
    slot_index = jnp.sum(earlier * one_hot, axis=2)
    block_index = jnp.arange(col_total, dtype=jnp.int32)[:, None]
    home_row = 2 * ids_rows // col_total
    mine = (2 * ids_rows % col_total) // 2 == col_index // 2
    step = (home_row - row_index + row_total) % row_total
    position = (step * col_total + block_index) * capacity + slot_index
    position = jnp.where(mine, position, -1).reshape(seq_len)
    slot_count = row_total * col_total * capacity
    slots = jnp.arange(slot_count, dtype=jnp.int32)
    placing = (slots[:, None] == position[None, :]).astype(jnp.bfloat16)
    picking = (position[:, None] == slots[None, :]).astype(jnp.bfloat16)

    table = matmul(placing, normed_image).astype(jnp.bfloat16)
    table = table.reshape(row_total, col_total * capacity, model_width)
    expert_rows, hidden_units = exchange(
        "dispatch", 3, shuffles=((table, 1),), units=((normed_image, up_whole, True),)
    )
    expert_units = up_gelu(expert_rows.reshape(slot_count, model_width), expert_in[0])
    partial_out = matmul(expert_units, expert_out[0]).astype(jnp.bfloat16)
    partial_out = partial_out.reshape(row_total, col_total * capacity, model_width)
    returned, dense_part = exchange(
        "collect", 4, shuffles=((partial_out, -1),), units=((hidden_units, down_whole, False),)
    )

    rows_two = returned.reshape(slot_count, model_width)
    partial = dense_part.astype(jnp.float32) + matmul(picking, rows_two)
    partial = partial.astype(jnp.bfloat16).reshape(col_total, tok_count, model_width)
    (total,) = exchange("leave", 5, sums=(partial,))
    return (hidden_mine.astype(jnp.float32) + total).astype(jnp.bfloat16)


def solution(mesh):
    in_specs = (
        P(("row", "col"), None),
        P(),
        P("row", "col", None, None),
        P("col", "row"),
        P(),
        P("row", "col"),
        P("col", "row"),
        P(("row", "col"), None),
        P(("row", "col"), None, None),
        P(("row", "col"), None, None),
    )
    out_specs = P(("row", "col"), None)
    return jax.shard_map(shards, mesh=mesh, in_specs=in_specs, out_specs=out_specs, check_vma=False)
```
